32 devices in a mesh: lat: 4 (over x, core), lon: 8 (over z, y).
Axes of the slice: x: 2, y: 2, z: 4, core: 2. Of those that a mesh axis runs over, the one named last changes fastest.
Arguments:
- tokens: bfloat16 [4, 56, 32, 1536], P(None, 'lat', 'lon'), may hold values from -400 to 400, as said below
- in_bounds: int32 [5], replicated, may hold values from 0 to 47, as said below
- out_bounds: int32 [5], replicated, may hold values from 0 to 24, as said below
- down_gain: float32 [768], replicated, may hold values from 0.25 to 1.75
- down_bias: float32 [768], replicated, may hold values from -1 to 1
- down_weight: bfloat16 [768, 384], replicated, may hold values from -0.21875 to 0.21875
- up_weight: bfloat16 [384, 768], replicated, may hold values from -0.3125 to 0.3125
- up_gain: float32 [192], replicated, may hold values from 0.25 to 1.75
- up_bias: float32 [192], replicated, may hold values from -1 to 1
- out_weight: bfloat16 [192, 192], replicated, may hold values from -0.4375 to 0.4375
Outputs:
- merged: bfloat16 [4, 32, 16, 3072], P(None, 'lat', 'lon')
- upsampled: bfloat16 [4, 56, 32, 1536], P(None, 'lat', 'lon')
The draws below stay inside these ranges and needn't reach their ends.
Inputs may be any that keep to these rules, and one draw needn't show every extreme that they name: `tokens`: band b's fine rows stand in its slots from the first one on; slots past the band's count hold values that no output reads. in_bounds[0] = 0, in_bounds[4] = 47; each band has 10 to 14 fine rows, and some band has 14. out_bounds[0] = 0, out_bounds[4] = 24; each band has 4 to 8 merged rows, and some band has 8. For 0 < b < 4, 2 * out_bounds[b] - in_bounds[b] is 1 to 3, and 3 for some b; so merged band b covers fine rows from band b's first on to at most 3 rows past its last (fine row 47 counting as zeros), and band b's fine rows need merged rows from at most 2 rows before merged band b's first up to its last, 2 being reached.
All inputs are finite; a program needn't handle non-finite values.
Results may differ from the reference program's by a relative error of at most 0.0069.
Values may be sent and summed in bfloat16 or wider, within the bound.
A program may use at most 64 MiB of HBM per device.

```python
import math
import jax
import jax.numpy as jnp
from jax import lax

C = 192
LEV = 8
ROWS_DEV = 12
LON_DEV = 4
MEMBERS = 4
LCAP = 14
MCAP = 8
LAT = 47
MLAT = 24
LON = 32
N_LAT = 4
N_LON = 8


def pick_three(pattern, first, second, third):
    return jnp.where(pattern == 0, first, jnp.where(pattern == 1, second, third))


def bound_pair(key):
    base_key = jax.random.fold_in(key, 11)
    key_index, key_pattern, key_extra = jax.random.split(base_key, 3)
    places = jnp.arange(N_LAT + 1, dtype=jnp.int32)
    coarse_table = jnp.array([0, 1, 1, 1, 2], jnp.int32)
    fine_table = jnp.array([-1, -1, 0, 1, 1], jnp.int32)
    choose = jax.random.randint(key_index, (N_LAT + 1,), 0, 5).astype(jnp.int32)
    coarse_moves = jnp.take(coarse_table, choose)
    fine_moves = jnp.take(fine_table, choose)
    pattern = jax.random.randint(key_pattern, (), 0, 3).astype(jnp.int32)
    extra = jax.random.randint(key_extra, (), -1, 2).astype(jnp.int32)
    coarse_one = pick_three(pattern, 0, 2, coarse_moves[1])
    fine_one = pick_three(pattern, -1, 1, fine_moves[1])
    coarse_two = pick_three(pattern, 2, 0, 0)
    fine_two = pick_three(pattern, 1, -1, -1)
    coarse_three = pick_three(pattern, 1, jnp.where(extra > 0, 2, 1), 2)
    fine_three = pick_three(pattern, extra, 1, 1)
    coarse_moves = jnp.where(places == 1, coarse_one, jnp.where(places == 2, coarse_two, jnp.where(places == 3, coarse_three, coarse_moves)))
    fine_moves = jnp.where(places == 1, fine_one, jnp.where(places == 2, fine_two, jnp.where(places == 3, fine_three, fine_moves)))
    edges = (places == 0) | (places == N_LAT)
    fine_moves = jnp.where(edges, 0, fine_moves)
    coarse_moves = jnp.where(edges, 0, coarse_moves)
    fine_bounds = places * ROWS_DEV + fine_moves
    fine_bounds = jnp.where(places == N_LAT, N_LAT * ROWS_DEV - 1, fine_bounds)
    coarse_bounds = places * (ROWS_DEV // 2) + coarse_moves
    return (fine_bounds.astype(jnp.int32), coarse_bounds.astype(jnp.int32))


def draw_in_bounds(key, part):
    return bound_pair(key)[0]


def draw_out_bounds(key, part):
    return bound_pair(key)[1]


def draw_tokens(key, part):
    key_base, key_rows, key_chan = jax.random.split(jax.random.fold_in(key, 5), 3)
    shape = (MEMBERS, N_LAT * (ROWS_DEV + 2), LON_DEV * N_LON, LEV * C)
    row_scale = jnp.exp(jax.random.uniform(key_rows, (MEMBERS, N_LAT * (ROWS_DEV + 2), LON_DEV * N_LON, 1), jnp.float32, 0.0, math.log(10.0)))
    chan_scale = jnp.exp(jax.random.uniform(key_chan, (1, 1, 1, LEV * C), jnp.float32, 0.0, math.log(10.0)))
    values = jnp.clip(jax.random.normal(key_base, shape, jnp.float32), -4.0, 4.0)
    return (values * row_scale * chan_scale).astype(jnp.bfloat16)


def bell_draw(stream_key, shape, width, reach, kind=jnp.bfloat16):
    return jnp.clip(width * jax.random.normal(stream_key, shape, jnp.float32), -reach, reach).astype(kind)


def setup_inputs(seed: int = 0) -> dict:
    seeds = jax.random.split(jax.random.key(seed), 11)
    return {
        "tokens": draw_tokens(jax.random.fold_in(seeds[10], 71), 0),
        "in_bounds": draw_in_bounds(jax.random.fold_in(seeds[10], 71), 0),
        "out_bounds": draw_out_bounds(jax.random.fold_in(seeds[10], 71), 0),
        "down_gain": jnp.clip(1.0 + 0.15 * jax.random.normal(seeds[3], (4 * C,), jnp.float32), 0.25, 1.75),
        "down_bias": bell_draw(seeds[4], (4 * C,), 0.3, 1.0, jnp.float32),
        "down_weight": bell_draw(seeds[5], (4 * C, 2 * C), (4 * C) ** -0.5, 0.21875),
        "up_weight": bell_draw(seeds[6], (2 * C, 4 * C), (2 * C) ** -0.5, 0.3125),
        "up_gain": jnp.clip(1.0 + 0.15 * jax.random.normal(seeds[7], (C,), jnp.float32), 0.25, 1.75),
        "up_bias": bell_draw(seeds[8], (C,), 0.3, 1.0, jnp.float32),
        "out_weight": bell_draw(seeds[9], (C, C), C ** -0.5, 0.4375),
    }


def layer_norm(values, scale_vec, shift_vec):
    center = lax.optimization_barrier(jnp.mean(values, axis=-1, keepdims=True))
    spread = lax.optimization_barrier(jnp.mean(jnp.square(values - center), axis=-1, keepdims=True))
    return (values - center) * lax.rsqrt(spread + 1e-05) * scale_vec + shift_vec

def reference(tokens, in_bounds, out_bounds, down_gain, down_bias, down_weight, up_weight, up_gain, up_bias, out_weight):
    half_lon = LON // 2
    lat_rows = jnp.arange(LAT, dtype=jnp.int32)
    band_of = lax.optimization_barrier(jnp.sum((lat_rows[:, None] >= in_bounds[None, 1:N_LAT]).astype(jnp.int32), axis=1)).astype(jnp.int32)
    slot_of = (band_of * LCAP + lat_rows - in_bounds[band_of]).astype(jnp.int32)

    def one_member(member):
        token_grid = jnp.take(member, slot_of, axis=0)
        token_grid = jnp.concatenate([token_grid, jnp.zeros((1, LON, LEV * C), jnp.bfloat16)], axis=0)
        token_grid = jnp.roll(token_grid, 1, axis=1)
        pieces = token_grid.reshape(MLAT, 2, half_lon, 2, LEV, C).transpose(0, 2, 4, 3, 1, 5).reshape(-1, 4 * C)
        normed = layer_norm(pieces.astype(jnp.float32), down_gain, down_bias).astype(jnp.bfloat16)
        coarse = jnp.dot(normed, down_weight, preferred_element_type=jnp.float32).astype(jnp.bfloat16)
        widened = jnp.dot(coarse, up_weight, preferred_element_type=jnp.float32).astype(jnp.bfloat16)
        widened = widened.reshape(MLAT, half_lon, LEV, 2, 2, C).transpose(0, 4, 1, 3, 2, 5).reshape(2 * MLAT, LON, LEV, C)
        widened = jnp.roll(widened, -1, axis=1)[:LAT]
        renormed = layer_norm(widened.astype(jnp.float32), up_gain, up_bias).astype(jnp.bfloat16)
        finished = jnp.dot(renormed.reshape(-1, C), out_weight, preferred_element_type=jnp.float32).astype(jnp.bfloat16)
        return (coarse.reshape(MLAT, half_lon, LEV * 2 * C), finished.reshape(LAT, LON, LEV * C))
    coarse_all, fine_all = lax.map(one_member, tokens)
    fine_slots = jnp.arange(N_LAT * LCAP, dtype=jnp.int32)
    fine_band = (fine_slots // LCAP).astype(jnp.int32)
    fine_offset = (fine_slots % LCAP).astype(jnp.int32)
    fine_source = jnp.clip(in_bounds[fine_band] + fine_offset, 0, LAT - 1).astype(jnp.int32)
    fine_live = fine_offset < in_bounds[fine_band + 1] - in_bounds[fine_band]
    upsampled = jnp.where(fine_live[None, :, None, None], jnp.take(fine_all, fine_source, axis=1), jnp.zeros((), jnp.bfloat16))
    coarse_slots = jnp.arange(N_LAT * MCAP, dtype=jnp.int32)
    coarse_band = (coarse_slots // MCAP).astype(jnp.int32)
    coarse_offset = (coarse_slots % MCAP).astype(jnp.int32)
    coarse_source = jnp.clip(out_bounds[coarse_band] + coarse_offset, 0, MLAT - 1).astype(jnp.int32)
    coarse_live = coarse_offset < out_bounds[coarse_band + 1] - out_bounds[coarse_band]
    merged = jnp.where(coarse_live[None, :, None, None], jnp.take(coarse_all, coarse_source, axis=1), jnp.zeros((), jnp.bfloat16))
    return (merged.astype(jnp.bfloat16), upsampled.astype(jnp.bfloat16))
```

```python
import functools

import jax
import jax.numpy as jnp
from jax import lax
from jax.experimental import pallas as pl
from jax.experimental.pallas import tpu as pltpu
from jax.sharding import PartitionSpec as P

HALO = 3
LANES_OF_LEVELS = 4
TILE = 128
MESH = pl.DeviceIdType.MESH


def pair_norm(blocks, size):
    low = lax.broadcasted_iota(jnp.int32, blocks[0][0].shape, 1) < TILE // 2
    inv = 1.0 / size

    def totals(tiles):
        one, mid, two = [functools.reduce(jnp.add, group) for group in zip(*tiles)]
        first = jnp.sum(one + jnp.where(low, mid, 0.0), axis=1, keepdims=True) * inv
        second = jnp.sum(two + jnp.where(low, 0.0, mid), axis=1, keepdims=True) * inv
        return first, second

    first, second = totals(blocks)
    mid = jnp.where(low, first, second)
    off = [(one - first, both - mid, two - second) for one, both, two in blocks]
    first, second = totals([tuple(v * v for v in tiles) for tiles in off])
    first, second = lax.rsqrt(first + 1e-05), lax.rsqrt(second + 1e-05)
    mid = jnp.where(low, first, second)
    return low, [(one * first, both * mid, two * second) for one, both, two in off]


def down_pieces(chan):
    half = chan - TILE
    even = [(0, b * chan, TILE) for b in range(4)] + [(0, b * chan + TILE, half) for b in range(4)]
    odd = [(1, b * chan + half, TILE) for b in range(4)] + [(1, b * chan, half) for b in (1, 0, 3, 2)]
    return even + odd


def thirds(value):
    return tuple(value[:, t * TILE : (t + 1) * TILE] for t in range(3))


def kernel(
    n_lat,
    n_lon,
    in_b_hbm,
    out_b_hbm,
    t_hbm,
    dw_hbm,
    uw_hbm,
    ow_hbm,
    dg_hbm,
    db_hbm,
    ug_hbm,
    ub_hbm,
    mo_ref,
    fo_ref,
    comb,
    west_in,
    east_in,
    top_in,
    bot_in,
    top_w,
    top_e,
    bot_w,
    bot_e,
    tail,
    tail_w,
    tail_e,
    nrm,
    coarse,
    renorm,
    turn_in,
    turn_merged,
    turn_fine,
    dw,
    uw,
    ow,
    ow_pad,
    down_vec,
    up_vec,
    t_ref,
    in_b,
    out_b,
    dg_ref,
    db_ref,
    ug_ref,
    ub_ref,
    local_sem,
    send_sem,
    recv_sem,
    wrap_sem,
):
    members, slots, cols, packed = t_ref.shape
    merged_slots = mo_ref.shape[1]
    _, _, sub, lanes = comb.shape
    halves = sub // members
    tiles = lanes // TILE
    total = slots + 2 * HALO
    rows = 2 * merged_slots + 4
    mid_lo, mid_hi = HALO, slots // 2
    lat = lax.axis_index("lat")
    lon = lax.axis_index("lon")
    east = {"lat": lat, "lon": lax.rem(lon + 1, n_lon)}
    west = {"lat": lat, "lon": lax.rem(lon + n_lon - 1, n_lon)}
    above = {"lat": jnp.maximum(lat - 1, 0), "lon": lon}
    below = {"lat": jnp.minimum(lat + 1, n_lat - 1), "lon": lon}
    has_above = lat > 0
    has_below = lat < n_lat - 1

    first = lon == 0
    last = lon == n_lon - 1
    barrier = pltpu.get_barrier_semaphore()
    pl.semaphore_signal(barrier, inc=1, device_id=west, device_id_type=MESH)

    @pl.when(jnp.logical_not(last))
    def _():
        pl.semaphore_signal(barrier, inc=1, device_id=east, device_id_type=MESH)

    @pl.when(has_above)
    def _():
        pl.semaphore_signal(barrier, inc=1, device_id=above, device_id_type=MESH)

    @pl.when(has_below)
    def _():
        pl.semaphore_signal(barrier, inc=1, device_id=below, device_id_type=MESH)

    pairs = [
        (t_hbm, t_ref),
        (in_b_hbm, in_b),
        (out_b_hbm, out_b),
        (uw_hbm, uw),
        (ow_hbm, ow),
        (dg_hbm, dg_ref),
        (db_hbm, db_ref),
        (ug_hbm, ug_ref),
        (ub_hbm, ub_ref),
    ]
    chan = lanes // LANES_OF_LEVELS
    short = chan - TILE
    for pos, (e, start, size) in enumerate(down_pieces(chan)):
        at = sum(piece[2] for piece in down_pieces(chan)[:pos] if piece[0] == e)
        pairs.append((dw_hbm.at[pl.ds(start, size)], dw.at[e, pl.ds(at, size)]))
    loads = [pltpu.make_async_copy(src, dst, local_sem.at[i]) for i, (src, dst) in enumerate(pairs)]
    for load in loads:
        load.start()
    loads[0].wait()

    for r in range(slots):
        for member in range(members):
            row = t_ref[member, r].astype(jnp.float32)
            for half in range(halves):
                at = (half * members + member) * cols
                for t in range(tiles):
                    lane = half * lanes + t * TILE
                    turn_in[r, t, at : at + cols, :] = row[:, lane : lane + TILE]

    def take_column(x):
        for r in range(slots):
            for t in range(tiles):
                comb[1 + x, HALO + r, :, t * TILE : (t + 1) * TILE] = turn_in[
                    r, t, pl.ds(x, sub, stride=cols), :
                ].astype(jnp.bfloat16)

    take_column(cols - 1)
    take_column(0)

    heard = 1 + jnp.logical_not(first).astype(jnp.int32)
    pl.semaphore_wait(barrier, heard + has_above.astype(jnp.int32) + has_below.astype(jnp.int32))

    @pl.when(last)
    def _():
        pl.semaphore_signal(wrap_sem, inc=1, device_id=east, device_id_type=MESH)

    def remote(src, dst, slot, device):
        return pltpu.make_async_remote_copy(
            src_ref=src,
            dst_ref=dst,
            send_sem=send_sem.at[slot],
            recv_sem=recv_sem.at[slot],
            device_id=device,
            device_id_type=MESH,
        )

    spans = [(0, mid_lo), (mid_hi, slots), (mid_lo, mid_hi)]
    to_east, to_west = [], []
    for i, (lo, hi) in enumerate(spans):
        span = pl.ds(lo, hi - lo)
        held = pl.ds(HALO + lo, hi - lo)
        to_east.append(remote(comb.at[cols, held], west_in.at[span], i, east))
        to_west.append(remote(comb.at[1, held], east_in.at[span], 3 + i, west))
    up = remote(comb.at[pl.ds(1, cols), pl.ds(HALO, HALO)], bot_in, 6, above)
    down = remote(tail, top_in, 7, below)
    head = pl.ds(0, HALO)
    up_w = remote(west_in.at[head], bot_w, 8, above)
    up_e = remote(east_in.at[head], bot_e, 9, above)
    down_w = remote(tail_w, top_w, 10, below)
    down_e = remote(tail_e, top_e, 11, below)

    @pl.when(last)
    def _():
        for copy in to_east + to_west:
            copy.start()

    @pl.when(jnp.logical_not(last | first))
    def _():
        for copy in to_west + to_east:
            copy.start()

    @pl.when(first)
    def _():
        for copy in to_east:
            copy.start()

    for x in range(1, cols - 1):
        take_column(x)

    @pl.when(has_above)
    def _():
        up.start()

    loads[1].wait()
    loads[2].wait()

    start_in = in_b[lat]
    end_in = in_b[lat + 1]
    count = end_in - start_in
    shift = 2 * out_b[lat] - start_in
    past = count - shift + 4

    for x in range(cols):
        for i in range(HALO):
            tail[x, i] = comb[1 + x, count + i]

    @pl.when(has_below)
    def _():
        down.start()

    for load in loads[3:]:
        load.wait()

    def place(r):
        inside = jnp.maximum(r + shift - 1, 0)
        outside = jnp.minimum(HALO + slots + r - past, total - 1)
        return jnp.where(r < past, inside, outside)

    spots = [place(r) for r in range(rows)]

    for e in range(2):
        for row, ref in ((0, dg_ref), (1, db_ref)):
            vec = ref[...][None]
            cuts = [vec[:, at : at + size] for which, at, size in down_pieces(chan) if which == e]
            down_vec[2 * e + row : 2 * e + row + 1, :] = jnp.concatenate(cuts, axis=1)
    for row, ref in ((0, ug_ref), (1, ub_ref)):
        vec = ref[...][None]
        up_vec[row : row + 1, :] = jnp.concatenate([vec, vec], axis=1)
    ow_pad[...] = jnp.zeros(ow_pad.shape, jnp.bfloat16)
    plain = ow[...]
    moved = jnp.concatenate([jnp.zeros((chan, short), jnp.bfloat16), plain], axis=1)
    for a in range(2):
        ow_pad[0, a, a * short : a * short + chan, 0:chan] = plain
        ow_pad[1, a, a * short : a * short + chan, :] = moved

    pairs_of_levels = LANES_OF_LEVELS // 2

    def compute(j, ms):
        nm = len(ms)
        part = nm * sub
        size = pairs_of_levels * part
        for k in range(0, nm, 2):
            for p in range(pairs_of_levels):
                cut = slice(p * 2 * chan, (p + 1) * 2 * chan)
                blocks = []
                for c in range(2):
                    for a in range(2):
                        rows_at = [comb[2 * j + c, spots[2 * m + a], :, cut] for m in ms[k : k + 2]]
                        blocks.append(thirds(jnp.concatenate([v.astype(jnp.float32) for v in rows_at], axis=0)))
                low, done = pair_norm(blocks, 4 * chan)
                even, odd = [v[0] for v in done], [v[2] for v in done]
                for b in (0, 2):
                    swapped = pltpu.roll(done[b + 1][1], TILE // 2, 1)
                    even.append(jnp.where(low, done[b][1], swapped))
                    odd.append(jnp.where(low, swapped, done[b][1]))
                for e, tiles_of in ((0, even), (1, odd)):
                    at = p * part + k * sub
                    for t, value in enumerate(tiles_of):
                        lane = slice(t * TILE, (t + 1) * TILE)
                        value = value * down_vec[2 * e : 2 * e + 1, lane] + down_vec[2 * e + 1 : 2 * e + 2, lane]
                        nrm[e, at : at + 2 * sub, lane] = value.astype(jnp.bfloat16)
        for e in range(2):
            wide = jnp.dot(nrm[e, 0:size, :], dw[e], preferred_element_type=jnp.float32)
            coarse[e * size : (e + 1) * size, :] = wide.astype(jnp.bfloat16)
            if j < 2:
                for i, m in enumerate(ms):
                    if m < 2:
                        continue
                    for p in range(pairs_of_levels):
                        at = p * part + i * sub
                        for t in range(2 * chan // TILE):
                            turn_merged[
                                m - 2, (2 * p + e) * 2 * chan // TILE + t, pl.ds(j, sub, stride=cols // 2), :
                            ] = wide[at : at + sub, t * TILE : (t + 1) * TILE]
        for c, x in (((1, 0),), ((0, 1), (1, 2)), ((0, 3),))[j]:
            spread = jnp.dot(
                coarse[0 : 2 * size, :],
                uw[:, c * 2 * chan : (c + 1) * 2 * chan],
                preferred_element_type=jnp.float32,
            )
            for at in range(0, 2 * size, 2 * sub):
                _, done = pair_norm([thirds(spread[at : at + 2 * sub])], chan)
                for t, value in enumerate(done[0]):
                    lane = slice(t * TILE, (t + 1) * TILE)
                    value = value * up_vec[0:1, lane] + up_vec[1:2, lane]
                    renorm[at : at + 2 * sub, lane] = value.astype(jnp.bfloat16)
            for a in range(2):
                two = [
                    jnp.dot(
                        renorm[e * size : (e + 1) * size, a * TILE : (a + 2) * TILE],
                        ow_pad[e, a],
                        preferred_element_type=jnp.float32,
                    )
                    for e in range(2)
                ]
                for i, m in enumerate(ms):
                    for p in range(pairs_of_levels):
                        span = slice(p * part + i * sub, p * part + (i + 1) * sub)
                        trio = (
                            two[0][span, 0:TILE],
                            two[0][span, TILE : 2 * TILE] + two[1][span, 0:TILE],
                            two[1][span, TILE : 2 * TILE],
                        )
                        for t, value in enumerate(trio):
                            turn_fine[2 * m + a, 3 * p + t, pl.ds(x, sub, stride=cols), :] = value

    own = pl.ds(1, cols)

    @pl.when(has_above)
    def _():
        down.wait_recv()

    @pl.when(has_below)
    def _():
        up.wait_recv()
        comb[own, HALO + slots : total] = bot_in[...]

    @pl.when(jnp.logical_not(has_below))
    def _():
        comb[:, HALO + slots : total] = jnp.zeros((cols + 2, HALO, sub, lanes), jnp.bfloat16)

    @pl.when(has_above)
    def _():
        comb[own, 0:HALO] = top_in[...]

    @pl.when(jnp.logical_not(has_above))
    def _():
        comb[:, 0:HALO] = jnp.zeros((cols + 2, HALO, sub, lanes), jnp.bfloat16)

    merged_rows = rows // 2
    with jax.named_scope("s_c1"):
        compute(1, list(range(merged_rows)))

    @pl.when(first)
    def _():
        pl.semaphore_wait(wrap_sem, 1)
        for copy in to_west:
            copy.start()

    def arrive(copies, landed, x, tail_x, up_x, down_x, top_x, bot_x):
        for i in range(2):
            lo, hi = spans[i]
            copies[i].wait_recv()
            comb[x, HALO + lo : HALO + hi] = landed[lo:hi]
        for i in range(HALO):
            tail_x[i] = comb[x, count + i]

        @pl.when(has_above)
        def _():
            up_x.start()

        @pl.when(has_below)
        def _():
            down_x.start()

        lo, hi = spans[2]
        copies[2].wait_recv()
        comb[x, HALO + lo : HALO + hi] = landed[lo:hi]

    def corners(x, up_x, down_x, top_x, bot_x):
        @pl.when(has_above)
        def _():
            down_x.wait_recv()
            comb[x, 0:HALO] = top_x[...]

        @pl.when(has_below)
        def _():
            up_x.wait_recv()
            comb[x, HALO + slots : total] = bot_x[...]

    with jax.named_scope("s_aW"):
        arrive(to_west, east_in, cols + 1, tail_e, up_e, down_e, top_e, bot_e)
    with jax.named_scope("s_cW"):
        corners(cols + 1, up_e, down_e, top_e, bot_e)
    with jax.named_scope("s_c2"):
        compute(2, list(range(merged_rows)))
    with jax.named_scope("s_aE"):
        arrive(to_east, west_in, 0, tail_w, up_w, down_w, top_w, bot_w)
    with jax.named_scope("s_cE"):
        corners(0, up_w, down_w, top_w, bot_w)

    def put_out(value, live, slot, out_ref, width, span):
        value = jnp.where(live, value, 0.0).astype(jnp.bfloat16)
        for half in range(halves):
            for member in range(members):
                at = (half * members + member) * width
                out_ref[member, slot, :, half * span : (half + 1) * span] = jnp.concatenate(
                    [value[t, at : at + width] for t in range(span // TILE)], axis=1
                )

    with jax.named_scope("s_c0"):
        compute(0, list(range(merged_rows)))
    count_out = out_b[lat + 1] - out_b[lat]
    for m in range(merged_slots):
        put_out(turn_merged[m], m < count_out, m, mo_ref, cols // 2, 2 * lanes)
    for k in range(slots):
        put_out(turn_fine[4 - shift + k], k < count, k, fo_ref, cols, lanes)

    for copy in to_east + to_west:
        copy.wait_send()

    @pl.when(has_above)
    def _():
        up.wait_send()
        up_w.wait_send()
        up_e.wait_send()

    @pl.when(has_below)
    def _():
        down.wait_send()
        down_w.wait_send()
        down_e.wait_send()


def write_out(merged_ref, fine_ref, merged_hbm, fine_hbm, sem):
    copies = [
        pltpu.make_async_copy(merged_ref, merged_hbm, sem.at[0]),
        pltpu.make_async_copy(fine_ref, fine_hbm, sem.at[1]),
    ]
    for copy in copies:
        copy.start()
    for copy in copies:
        copy.wait()


def body(
    tokens,
    in_bounds,
    out_bounds,
    down_gain,
    down_bias,
    down_weight,
    up_weight,
    up_gain,
    up_bias,
    out_weight,
):
    members, slots, cols, packed = tokens.shape
    chan = down_weight.shape[0] // 4
    halves = packed // (chan * LANES_OF_LEVELS)
    lanes = chan * LANES_OF_LEVELS
    sub = halves * members
    merged_slots = slots // 2 + 1
    half_cols = cols // 2
    rows = 2 * merged_slots + 4
    total = slots + 2 * HALO
    bf16 = jnp.bfloat16
    n_lat = lax.axis_size("lat")
    n_lon = lax.axis_size("lon")
    vmem = pl.BlockSpec(memory_space=pltpu.VMEM)
    hbm = pl.BlockSpec(memory_space=pltpu.HBM)
    column = pltpu.VMEM((slots, sub, lanes), bf16)
    patch = pltpu.VMEM((cols, HALO, sub, lanes), bf16)
    corner = pltpu.VMEM((HALO, sub, lanes), bf16)
    operands = (
        in_bounds,
        out_bounds,
        tokens,
        down_weight,
        up_weight,
        out_weight,
        down_gain,
        down_bias,
        up_gain,
        up_bias,
    )
    merged_shape = (members, merged_slots, half_cols, 2 * packed)
    held = pl.pallas_call(
        functools.partial(kernel, n_lat, n_lon),
        out_shape=(pltpu.VMEM(merged_shape, bf16), pltpu.VMEM(tokens.shape, bf16)),
        in_specs=[hbm] * 10,
        out_specs=(vmem, vmem),
        scratch_shapes=[
            pltpu.VMEM((cols + 2, total, sub, lanes), bf16),
            column,
            column,
            patch,
            patch,
            corner,
            corner,
            corner,
            corner,
            patch,
            corner,
            corner,
            pltpu.VMEM((2, LANES_OF_LEVELS * rows // 4 * sub, 4 * chan), bf16),
            pltpu.VMEM((LANES_OF_LEVELS * rows // 2 * sub, 2 * chan), bf16),
            pltpu.VMEM((LANES_OF_LEVELS * rows // 2 * sub, 2 * chan), bf16),
            pltpu.VMEM((slots, lanes // TILE, sub * cols, TILE), jnp.float32),
            pltpu.VMEM((merged_slots, 2 * lanes // TILE, sub * half_cols, TILE), jnp.float32),
            pltpu.VMEM((rows, lanes // TILE, sub * cols, TILE), jnp.float32),
            pltpu.VMEM((2, *down_weight.shape), bf16),
            pltpu.VMEM(up_weight.shape, bf16),
            pltpu.VMEM(out_weight.shape, bf16),
            pltpu.VMEM((2, 2, 2 * TILE, 2 * TILE), bf16),
            pltpu.VMEM((4, 4 * chan), jnp.float32),
            pltpu.VMEM((2, 2 * chan), jnp.float32),
            pltpu.VMEM(tokens.shape, bf16),
            pltpu.SMEM(in_bounds.shape, jnp.int32),
            pltpu.SMEM(out_bounds.shape, jnp.int32),
            pltpu.VMEM(down_gain.shape, jnp.float32),
            pltpu.VMEM(down_bias.shape, jnp.float32),
            pltpu.VMEM(up_gain.shape, jnp.float32),
            pltpu.VMEM(up_bias.shape, jnp.float32),
            pltpu.SemaphoreType.DMA((9 + len(down_pieces(chan)),)),
            pltpu.SemaphoreType.DMA((12,)),
            pltpu.SemaphoreType.DMA((12,)),
            pltpu.SemaphoreType.REGULAR,
        ],
        compiler_params=pltpu.CompilerParams(
            collective_id=0, has_side_effects=True, vmem_limit_bytes=48 * 2**20
        ),
    )(*[pltpu.with_memory_space_constraint(x, pltpu.HBM) for x in operands])
    return pl.pallas_call(
        write_out,
        out_shape=(
            jax.ShapeDtypeStruct(merged_shape, bf16),
            jax.ShapeDtypeStruct(tokens.shape, bf16),
        ),
        in_specs=[vmem, vmem],
        out_specs=(hbm, hbm),
        scratch_shapes=[pltpu.SemaphoreType.DMA((2,))],
    )(*[pltpu.with_memory_space_constraint(x, pltpu.VMEM) for x in held])


def solution(mesh):
    return jax.shard_map(
        body,
        mesh=mesh,
        in_specs=(P(None, "lat", "lon", None), P(), P(), P(), P(), P(), P(), P(), P(), P()),
        out_specs=(P(None, "lat", "lon", None), P(None, "lat", "lon", None)),
        check_vma=False,
    )
```

```python
import functools

import jax
import jax.numpy as jnp
from jax import lax
from jax.experimental import pallas as pl
from jax.experimental.pallas import tpu as pltpu
from jax.sharding import PartitionSpec as P

HALO = 3
LANES_OF_LEVELS = 4
PAIRS = LANES_OF_LEVELS // 2
TILE = 128
TOP = 2
BOTTOM = 2
WEST, EAST = 0, 1
MESH = pl.DeviceIdType.MESH
F32 = jnp.float32
BF16 = jnp.bfloat16


def pair_norm(blocks, size):
    low = lax.broadcasted_iota(jnp.int32, blocks[0][0].shape, 1) < TILE // 2
    inv = 1.0 / size

    def totals(tiles):
        one, mid, two = [functools.reduce(jnp.add, group) for group in zip(*tiles)]
        first = jnp.sum(one + jnp.where(low, mid, 0.0), axis=1, keepdims=True) * inv
        second = jnp.sum(two + jnp.where(low, 0.0, mid), axis=1, keepdims=True) * inv
        return first, second

    first, second = totals(blocks)
    mid = jnp.where(low, first, second)
    off = [(one - first, both - mid, two - second) for one, both, two in blocks]
    first, second = totals([tuple(v * v for v in tiles) for tiles in off])
    first, second = lax.rsqrt(first + 1e-05), lax.rsqrt(second + 1e-05)
    mid = jnp.where(low, first, second)
    return low, [(one * first, both * mid, two * second) for one, both, two in off]


def thirds(value):
    return tuple(value[:, t * TILE : (t + 1) * TILE] for t in range(3))


def down_pieces(chan):
    short = chan - TILE
    even = [(0, b * chan, TILE) for b in range(4)] + [(0, b * chan + TILE, short) for b in range(4)]
    odd = [(1, b * chan + short, TILE) for b in range(4)] + [(1, b * chan, short) for b in (1, 0, 3, 2)]
    return even + odd


def kernel(
    n_lat,
    n_lon,
    in_b_hbm,
    out_b_hbm,
    t_hbm,
    dw_hbm,
    uw_hbm,
    ow_hbm,
    dg_hbm,
    db_hbm,
    ug_hbm,
    ub_hbm,
    turn_merged,
    turn_fine,
    places,
    comb,
    land,
    top_in,
    bot_in,
    top_side,
    bot_side,
    tail,
    tail_side,
    nrm,
    coarse,
    renorm,
    turn_in,
    dw,
    uw,
    ow,
    ow_pad,
    down_vec,
    up_vec,
    t_ref,
    in_b,
    out_b,
    dg_ref,
    db_ref,
    ug_ref,
    ub_ref,
    local_sem,
    send_sem,
    recv_sem,
    wrap_sem,
):
    members, slots, cols, packed = t_ref.shape
    _, _, sub, lanes = comb.shape
    halves = sub // members
    chan = lanes // LANES_OF_LEVELS
    short = chan - TILE
    tiles = lanes // TILE
    total = slots + 2 * HALO
    half_cols = cols // 2
    inner = slots // 2
    mid_lo, mid_hi = HALO, slots // 2
    lat = lax.axis_index("lat")
    lon = lax.axis_index("lon")
    east = {"lat": lat, "lon": lax.rem(lon + 1, n_lon)}
    west = {"lat": lat, "lon": lax.rem(lon + n_lon - 1, n_lon)}
    above = {"lat": jnp.maximum(lat - 1, 0), "lon": lon}
    below = {"lat": jnp.minimum(lat + 1, n_lat - 1), "lon": lon}
    has_above = lat > 0
    has_below = lat < n_lat - 1
    first = lon == 0
    last = lon == n_lon - 1

    barrier = pltpu.get_barrier_semaphore()
    pl.semaphore_signal(barrier, inc=1, device_id=west, device_id_type=MESH)

    @pl.when(jnp.logical_not(last))
    def _():
        pl.semaphore_signal(barrier, inc=1, device_id=east, device_id_type=MESH)

    @pl.when(has_above)
    def _():
        pl.semaphore_signal(barrier, inc=1, device_id=above, device_id_type=MESH)

    @pl.when(has_below)
    def _():
        pl.semaphore_signal(barrier, inc=1, device_id=below, device_id_type=MESH)

    pairs = [
        (t_hbm, t_ref),
        (in_b_hbm, in_b),
        (out_b_hbm, out_b),
        (ow_hbm, ow),
        (dg_hbm, dg_ref),
        (db_hbm, db_ref),
        (ug_hbm, ug_ref),
        (ub_hbm, ub_ref),
    ]
    loads = [pltpu.make_async_copy(src, dst, local_sem.at[i]) for i, (src, dst) in enumerate(pairs)]
    for load in loads:
        load.start()
    for block in range(2):
        cut = uw_hbm.at[:, pl.ds(block * 2 * chan, 2 * chan)]
        pltpu.make_async_copy(cut, uw.at[block], local_sem.at[len(pairs)]).start()
    for pos, (e, start, size) in enumerate(down_pieces(chan)):
        at = sum(piece[2] for piece in down_pieces(chan)[:pos] if piece[0] == e)
        cut = dw_hbm.at[pl.ds(start, size)]
        pltpu.make_async_copy(cut, dw.at[e, pl.ds(at, size)], local_sem.at[len(pairs) + 1]).start()
    loads[0].wait()

    for r in range(slots):
        for member in range(members):
            row = t_ref[member, r].astype(F32)
            for half in range(halves):
                at = (half * members + member) * cols
                for t in range(tiles):
                    lane = half * lanes + t * TILE
                    turn_in[r, t, at : at + cols, :] = row[:, lane : lane + TILE]

    for x in range(cols):
        for r in range(slots):
            for t in range(tiles):
                comb[1 + x, HALO + r, :, t * TILE : (t + 1) * TILE] = turn_in[
                    r, t, pl.ds(x, sub, stride=cols), :
                ].astype(BF16)

    loads[1].wait()
    loads[2].wait()
    start_in = in_b[lat]
    count = in_b[lat + 1] - start_in
    shift = 2 * out_b[lat] - start_in
    past = count - shift + 2 * TOP
    edge = past // 2
    places[0] = count
    places[1] = shift
    places[2] = edge
    places[3] = out_b[lat + 1] - out_b[lat]
    for x in range(cols):
        for i in range(HALO):
            tail[x, i] = comb[1 + x, count + i]

    heard = 1 + jnp.logical_not(first).astype(jnp.int32)
    pl.semaphore_wait(barrier, heard + has_above.astype(jnp.int32) + has_below.astype(jnp.int32))

    @pl.when(last)
    def _():
        pl.semaphore_signal(wrap_sem, inc=1, device_id=east, device_id_type=MESH)

    def remote(src, dst, slot, device):
        return pltpu.make_async_remote_copy(
            src_ref=src,
            dst_ref=dst,
            send_sem=send_sem.at[slot],
            recv_sem=recv_sem.at[slot],
            device_id=device,
            device_id_type=MESH,
        )

    spans = [(0, mid_lo), (mid_hi, slots), (mid_lo, mid_hi)]

    def column(side, x, i, device):
        lo, hi = spans[i]
        span = pl.ds(lo, hi - lo)
        return remote(comb.at[x, pl.ds(HALO + lo, hi - lo)], land.at[side, span], 3 * side + i, device)

    to_east = [column(WEST, cols, i, east) for i in range(3)]
    to_west = [column(EAST, 1, i, west) for i in range(3)]
    up = remote(comb.at[pl.ds(1, cols), pl.ds(HALO, HALO)], bot_in, 6, above)
    down = remote(tail, top_in, 7, below)

    def up_side(side):
        return remote(land.at[side, pl.ds(0, HALO)], bot_side.at[side], 8 + side, above)

    def down_side(side):
        return remote(tail_side.at[side], top_side.at[side], 10 + side, below)

    @pl.when(has_above)
    def _():
        up.start()

    @pl.when(has_below)
    def _():
        down.start()

    @pl.when(jnp.logical_not(last))
    def _():
        for copy in to_east:
            copy.start()

    @pl.when(jnp.logical_not(first))
    def _():
        for copy in to_west:
            copy.start()

    for load in loads[3:]:
        load.wait()
    pltpu.make_async_copy(uw, uw, local_sem.at[len(pairs)]).wait()
    pltpu.make_async_copy(dw, dw, local_sem.at[len(pairs) + 1]).wait()

    for e in range(2):
        for row, ref in ((0, dg_ref), (1, db_ref)):
            vec = ref[...][None]
            cuts = [vec[:, at : at + size] for which, at, size in down_pieces(chan) if which == e]
            down_vec[2 * e + row : 2 * e + row + 1, :] = jnp.concatenate(cuts, axis=1)
    for row, ref in ((0, ug_ref), (1, ub_ref)):
        vec = ref[...][None]
        up_vec[row : row + 1, :] = jnp.concatenate([vec, vec], axis=1)
    ow_pad[...] = jnp.zeros(ow_pad.shape, BF16)
    plain = ow[...]
    moved = jnp.concatenate([jnp.zeros((chan, short), BF16), plain], axis=1)
    for a in range(2):
        ow_pad[0, a, a * short : a * short + chan, 0:chan] = plain
        ow_pad[1, a, a * short : a * short + chan, :] = moved

    turn_fine[2 * (TOP + inner + BOTTOM)] = jnp.zeros(turn_fine.shape[1:], F32)
    turn_merged[inner + BOTTOM] = jnp.zeros(turn_merged.shape[1:], F32)

    def place(r):
        inside = jnp.maximum(r + shift - 1, 0)
        outside = jnp.minimum(HALO + slots + r - past, total - 1)
        return jnp.where(r < past, inside, outside)

    top_rows = [([place(2 * m + a) for a in range(2)], 2 * m, None) for m in range(TOP)]
    inner_rows = [([2 * m + a + shift - 1 for a in range(2)], 2 * m, m - TOP) for m in range(TOP, TOP + inner)]
    bottom_rows = [
        ([place(2 * (edge + i) + a) for a in range(2)], 2 * (TOP + inner + i), inner + i) for i in range(BOTTOM)
    ]
    step = PAIRS * sub

    def compute(cells, ups, skip=0):
        n = len(cells)
        size = n * step
        groups = sorted({(lo, hi) for lo, hi, _, _ in ups})

        def coarse_at(i, e):
            lo, hi = next(group for group in groups if group[0] <= i < group[1])
            return 2 * lo * step + e * (hi - lo) * step + (i - lo) * step

        for i, (col, _, (spots, _, _)) in enumerate(cells):
            blocks = []
            for c in range(2):
                for a in range(2):
                    row = comb[col + c, spots[a]].astype(F32)
                    both = [row[:, p * 2 * chan : (p + 1) * 2 * chan] for p in range(PAIRS)]
                    blocks.append(thirds(jnp.concatenate(both, axis=0)))
            low, done = pair_norm(blocks, 4 * chan)
            even, odd = [v[0] for v in done], [v[2] for v in done]
            for b in (0, 2):
                swapped = pltpu.roll(done[b + 1][1], TILE // 2, 1)
                even.append(jnp.where(low, done[b][1], swapped))
                odd.append(jnp.where(low, swapped, done[b][1]))
            for e, values in ((0, even), (1, odd)):
                for t, value in enumerate(values):
                    lane = slice(t * TILE, (t + 1) * TILE)
                    value = value * down_vec[2 * e : 2 * e + 1, lane] + down_vec[2 * e + 1 : 2 * e + 2, lane]
                    nrm[e, i * step : (i + 1) * step, lane] = value.astype(BF16)
        for e in range(2):
            wide = jnp.dot(nrm[e, 0:size, :], dw[e], preferred_element_type=F32)
            narrow = wide.astype(BF16)
            for i, (_, merged_col, (_, _, merged_at)) in enumerate(cells):
                coarse[coarse_at(i, e) : coarse_at(i, e) + step, :] = narrow[i * step : (i + 1) * step]
                if merged_col is None or merged_at is None:
                    continue
                for p in range(PAIRS):
                    at = i * step + p * sub
                    for t in range(3):
                        turn_merged[
                            merged_at + skip, (2 * p + e) * 3 + t, pl.ds(merged_col, sub, stride=half_cols), :
                        ] = wide[at : at + sub, t * TILE : (t + 1) * TILE]
        whole = sum(hi - lo for lo, hi, _, _ in ups) * step
        off = 0
        offs = []
        for lo, hi, block, _ in ups:
            part = (hi - lo) * step
            spread = jnp.dot(coarse[2 * lo * step : 2 * hi * step, :], uw[block], preferred_element_type=F32)
            for e in range(2):
                for at in range(0, part, step):
                    _, done = pair_norm([thirds(spread[e * part + at : e * part + at + step])], chan)
                    for t, value in enumerate(done[0]):
                        lane = slice(t * TILE, (t + 1) * TILE)
                        value = value * up_vec[0:1, lane] + up_vec[1:2, lane]
                        renorm[e * whole + off + at : e * whole + off + at + step, lane] = value.astype(BF16)
            offs.append(off)
            off += part
        for a in range(2):
            two = [
                jnp.dot(
                    renorm[e * whole : (e + 1) * whole, a * TILE : (a + 2) * TILE],
                    ow_pad[e, a],
                    preferred_element_type=F32,
                )
                for e in range(2)
            ]
            for (lo, hi, _, x), off in zip(ups, offs):
                for i in range(lo, hi):
                    _, _, (_, fine_at, _) = cells[i]
                    for p in range(PAIRS):
                        at = off + (i - lo) * step + p * sub
                        span = slice(at, at + sub)
                        trio = (
                            two[0][span, 0:TILE],
                            two[0][span, TILE : 2 * TILE] + two[1][span, 0:TILE],
                            two[1][span, TILE : 2 * TILE],
                        )
                        for t, value in enumerate(trio):
                            turn_fine[fine_at + a, 3 * p + t, pl.ds(x, sub, stride=cols), :] = value

    own = pl.ds(1, cols)

    with jax.named_scope("c_own_inner"):
        compute([(2, 1, row) for row in inner_rows], [(0, inner, 0, 1), (0, inner, 1, 2)])

    @pl.when(last)
    def _():
        for copy in to_east:
            copy.start()

    with jax.named_scope("w_halo"):

        @pl.when(has_above)
        def _():
            down.wait_recv()

        @pl.when(has_below)
        def _():
            up.wait_recv()
            comb[own, HALO + slots : total] = bot_in[...]

        @pl.when(jnp.logical_not(has_below))
        def _():
            comb[:, HALO + slots : total] = jnp.zeros((cols + 2, HALO, sub, lanes), BF16)

        @pl.when(has_above)
        def _():
            comb[own, 0:HALO] = top_in[...]

        @pl.when(jnp.logical_not(has_above))
        def _():
            comb[:, 0:HALO] = jnp.zeros((cols + 2, HALO, sub, lanes), BF16)

    with jax.named_scope("w_wrap"):

        @pl.when(first)
        def _():
            pl.semaphore_wait(wrap_sem, 1)
            for copy in to_west:
                copy.start()

    cross_lo = has_above & (lax.rem(lat, 2) == 0)
    cross_hi = has_below & (lax.rem(lat, 2) == 1)
    wrap_top_send = pltpu.make_async_remote_copy(
        src_ref=top_in.at[cols - 1],
        dst_ref=top_side.at[WEST],
        send_sem=send_sem.at[12],
        recv_sem=recv_sem.at[10 + WEST],
        device_id=east,
        device_id_type=MESH,
    )
    wrap_bot_send = pltpu.make_async_remote_copy(
        src_ref=bot_in.at[cols - 1],
        dst_ref=bot_side.at[WEST],
        send_sem=send_sem.at[12],
        recv_sem=recv_sem.at[8 + WEST],
        device_id=east,
        device_id_type=MESH,
    )

    @pl.when(last & cross_lo)
    def _():
        wrap_top_send.start()

    @pl.when(last & cross_hi)
    def _():
        wrap_bot_send.start()

    outer = top_rows + bottom_rows
    edges = len(outer)
    with jax.named_scope("c_own_outer"):
        compute([(2, 1, row) for row in outer], [(0, edges, 0, 1), (0, edges, 1, 2)])

    odd = lax.rem(lon, 2) == 1
    side_one = jnp.where(first | (odd & jnp.logical_not(last)), EAST, WEST)
    side_two = 1 - side_one

    def arrive(side):
        x = side * (cols + 1)
        for i in range(2):
            lo, hi = spans[i]
            column(side, cols, i, east).wait_recv()
            comb[x, HALO + lo : HALO + hi] = land[side, lo:hi]
        for i in range(HALO):
            tail_side[side, i] = comb[x, count + i]

        skip = first & (side == WEST)

        @pl.when(has_above & jnp.logical_not(skip & cross_lo))
        def _():
            up_side(side).start()

        @pl.when(has_below & jnp.logical_not(skip & cross_hi))
        def _():
            down_side(side).start()

        lo, hi = spans[2]
        column(side, cols, 2, east).wait_recv()
        comb[x, HALO + lo : HALO + hi] = land[side, lo:hi]


    def corner(side):
        x = side * (cols + 1)

        @pl.when(has_above)
        def _():
            down_side(side).wait_recv()
            comb[x, 0:HALO] = top_side[side]

        @pl.when(has_below)
        def _():
            up_side(side).wait_recv()
            comb[x, HALO + slots : total] = bot_side[side]

    side_rows = top_rows + inner_rows + bottom_rows
    for name, side in (("one", side_one), ("two", side_two)):
        with jax.named_scope("w_" + name):
            arrive(side)
        with jax.named_scope("k_" + name):
            corner(side)
        with jax.named_scope("c_" + name):
            compute(
                [(side * cols, 0, row) for row in side_rows],
                [(0, len(side_rows), 1 - side, side * (cols - 1))],
                skip=side * (inner + BOTTOM + 1),
            )

    for copy in to_east + to_west:
        copy.wait_send()

    @pl.when(has_above)
    def _():
        up.wait_send()
        up_side(EAST).wait_send()

    @pl.when(has_below)
    def _():
        down.wait_send()
        down_side(EAST).wait_send()

    @pl.when(has_above & jnp.logical_not(first & cross_lo))
    def _():
        up_side(WEST).wait_send()

    @pl.when(has_below & jnp.logical_not(first & cross_hi))
    def _():
        down_side(WEST).wait_send()

    @pl.when(last & (cross_lo | cross_hi))
    def _():
        wrap_top_send.wait_send()


def write_out(turn_merged, turn_fine, places, merged_hbm, fine_hbm, merged_buf, fine_buf, sem):
    members, merged_slots, half_cols, _ = merged_buf.shape
    _, slots, cols, packed = fine_buf.shape
    sub = turn_fine.shape[2] // cols
    halves = sub // members
    lanes = packed // halves
    inner = slots // 2
    count, shift, edge, count_out = places[0], places[1], places[2], places[3]
    copies = []

    def put(turn, index, slot, buf, width, span):
        value = turn[index].astype(BF16)
        for half in range(halves):
            for member in range(members):
                at = (half * members + member) * width
                buf[member, slot, :, half * span : (half + 1) * span] = jnp.concatenate(
                    [value[t, at : at + width] for t in range(span // TILE)], axis=1
                )

    def send(buf, hbm, lo, hi):
        span = pl.ds(lo, hi - lo)
        copy = pltpu.make_async_copy(buf.at[:, span], hbm.at[:, span], sem.at[len(copies)])
        copy.start()
        copies.append(copy)

    for lo in range(0, merged_slots, 4):
        hi = min(lo + 4, merged_slots)
        for slot in range(lo, hi):
            m = slot + TOP
            index = jnp.where(m < edge, slot, jnp.minimum(inner + m - edge, inner + BOTTOM - 1))
            index = jnp.where(slot < count_out, index, inner + BOTTOM)
            put(turn_merged, index, slot, merged_buf, half_cols, 2 * lanes)
        send(merged_buf, merged_hbm, lo, hi)
    for lo in range(0, slots, 5):
        hi = min(lo + 5, slots)
        for slot in range(lo, hi):
            r = slot + 2 * TOP - shift
            after = jnp.minimum(2 * (TOP + inner) + r - 2 * edge, 2 * (TOP + inner + BOTTOM) - 1)
            index = jnp.where(r < 2 * edge, r, after)
            index = jnp.where(slot < count, index, 2 * (TOP + inner + BOTTOM))
            put(turn_fine, index, slot, fine_buf, cols, lanes)
        send(fine_buf, fine_hbm, lo, hi)
    for copy in copies:
        copy.wait()


def body(
    tokens,
    in_bounds,
    out_bounds,
    down_gain,
    down_bias,
    down_weight,
    up_weight,
    up_gain,
    up_bias,
    out_weight,
):
    members, slots, cols, packed = tokens.shape
    chan = down_weight.shape[0] // 4
    halves = packed // (chan * LANES_OF_LEVELS)
    lanes = chan * LANES_OF_LEVELS
    sub = halves * members
    merged_slots = slots // 2 + 1
    half_cols = cols // 2
    inner = slots // 2
    edges = TOP + BOTTOM
    total = slots + 2 * HALO
    most = (inner + edges) * PAIRS * sub
    wide = max(2 * inner, inner + edges) * PAIRS * sub
    n_lat = lax.axis_size("lat")
    n_lon = lax.axis_size("lon")
    vmem = pl.BlockSpec(memory_space=pltpu.VMEM)
    smem = pl.BlockSpec(memory_space=pltpu.SMEM)
    hbm = pl.BlockSpec(memory_space=pltpu.HBM)
    patch = pltpu.VMEM((cols, HALO, sub, lanes), BF16)
    corner = pltpu.VMEM((2, HALO, sub, lanes), BF16)
    operands = (
        in_bounds,
        out_bounds,
        tokens,
        down_weight,
        up_weight,
        out_weight,
        down_gain,
        down_bias,
        up_gain,
        up_bias,
    )
    merged_shape = (members, merged_slots, half_cols, 2 * packed)
    held = pl.pallas_call(
        functools.partial(kernel, n_lat, n_lon),
        out_shape=(
            pltpu.VMEM((2 * (inner + BOTTOM) + 1, 2 * lanes // TILE, half_cols * sub, TILE), F32),
            pltpu.VMEM((2 * (TOP + inner + BOTTOM) + 1, lanes // TILE, cols * sub, TILE), F32),
            pltpu.SMEM((4,), jnp.int32),
        ),
        in_specs=[hbm] * 10,
        out_specs=(vmem, vmem, smem),
        scratch_shapes=[
            pltpu.VMEM((cols + 2, total, sub, lanes), BF16),
            pltpu.VMEM((2, slots, sub, lanes), BF16),
            patch,
            patch,
            corner,
            corner,
            patch,
            corner,
            pltpu.VMEM((2, most, 4 * chan), BF16),
            pltpu.VMEM((2 * most, 2 * chan), BF16),
            pltpu.VMEM((2 * wide, 2 * chan), BF16),
            pltpu.VMEM((slots, lanes // TILE, sub * cols, TILE), F32),
            pltpu.VMEM((2, *down_weight.shape), BF16),
            pltpu.VMEM((2, 2 * chan, 2 * chan), BF16),
            pltpu.VMEM(out_weight.shape, BF16),
            pltpu.VMEM((2, 2, 2 * TILE, 2 * TILE), BF16),
            pltpu.VMEM((4, 4 * chan), F32),
            pltpu.VMEM((2, 2 * chan), F32),
            pltpu.VMEM(tokens.shape, BF16),
            pltpu.SMEM(in_bounds.shape, jnp.int32),
            pltpu.SMEM(out_bounds.shape, jnp.int32),
            pltpu.VMEM(down_gain.shape, F32),
            pltpu.VMEM(down_bias.shape, F32),
            pltpu.VMEM(up_gain.shape, F32),
            pltpu.VMEM(up_bias.shape, F32),
            pltpu.SemaphoreType.DMA((10,)),
            pltpu.SemaphoreType.DMA((13,)),
            pltpu.SemaphoreType.DMA((12,)),
            pltpu.SemaphoreType.REGULAR,
        ],
        compiler_params=pltpu.CompilerParams(
            collective_id=0, has_side_effects=True, vmem_limit_bytes=48 * 2**20
        ),
    )(*[pltpu.with_memory_space_constraint(x, pltpu.HBM) for x in operands])
    spaces = (pltpu.VMEM, pltpu.VMEM, pltpu.SMEM)
    return pl.pallas_call(
        write_out,
        out_shape=(
            jax.ShapeDtypeStruct(merged_shape, BF16),
            jax.ShapeDtypeStruct(tokens.shape, BF16),
        ),
        in_specs=[vmem, vmem, smem],
        out_specs=(hbm, hbm),
        scratch_shapes=[
            pltpu.VMEM(merged_shape, BF16),
            pltpu.VMEM(tokens.shape, BF16),
            pltpu.SemaphoreType.DMA((pl.cdiv(merged_slots, 4) + pl.cdiv(slots, 5),)),
        ],
        compiler_params=pltpu.CompilerParams(vmem_limit_bytes=48 * 2**20),
    )(*[pltpu.with_memory_space_constraint(x, space) for x, space in zip(held, spaces)])


def solution(mesh):
    return jax.shard_map(
        body,
        mesh=mesh,
        in_specs=(P(None, "lat", "lon", None), P(), P(), P(), P(), P(), P(), P(), P(), P()),
        out_specs=(P(None, "lat", "lon", None), P(None, "lat", "lon", None)),
        check_vma=False,
    )
```

```python
import functools

import jax
import jax.numpy as jnp
from jax import lax
from jax.experimental import pallas as pl
from jax.experimental.pallas import tpu as pltpu
from jax.sharding import PartitionSpec as P

HALO = 3
LANES_OF_LEVELS = 4
PAIRS = LANES_OF_LEVELS // 2
TILE = 128
TOP = 2
BOTTOM = 2
WEST, EAST = 0, 1
MESH = pl.DeviceIdType.MESH
F32 = jnp.float32
BF16 = jnp.bfloat16
PARITIES = ((0, 1),)


def pair_norm(blocks, size):
    low = lax.broadcasted_iota(jnp.int32, blocks[0][0].shape, 1) < TILE // 2
    inv = 1.0 / size

    def totals(tiles):
        one, mid, two = [functools.reduce(jnp.add, group) for group in zip(*tiles)]
        first = jnp.sum(one + jnp.where(low, mid, 0.0), axis=1, keepdims=True) * inv
        second = jnp.sum(two + jnp.where(low, 0.0, mid), axis=1, keepdims=True) * inv
        return first, second

    first, second = totals(blocks)
    mid = jnp.where(low, first, second)
    off = [(one - first, both - mid, two - second) for one, both, two in blocks]
    first, second = totals([tuple(v * v for v in tiles) for tiles in off])
    first, second = lax.rsqrt(first + 1e-05), lax.rsqrt(second + 1e-05)
    mid = jnp.where(low, first, second)
    return low, [(one * first, both * mid, two * second) for one, both, two in off]


def thirds(value):
    return tuple(value[:, t * TILE : (t + 1) * TILE] for t in range(3))


def down_pieces(chan):
    short = chan - TILE
    even = [(0, b * chan, TILE) for b in range(4)] + [(0, b * chan + TILE, short) for b in range(4)]
    odd = [(1, b * chan + short, TILE) for b in range(4)] + [(1, b * chan, short) for b in (1, 0, 3, 2)]
    return even + odd


def kernel(
    n_lat,
    n_lon,
    in_b_hbm,
    out_b_hbm,
    t_hbm,
    dw_hbm,
    uw_hbm,
    ow_hbm,
    dg_hbm,
    db_hbm,
    ug_hbm,
    ub_hbm,
    turn_merged,
    turn_fine,
    places,
    comb,
    land,
    top_in,
    bot_in,
    top_side,
    bot_side,
    tail,
    tail_side,
    nrm,
    coarse,
    renorm,
    turn_in,
    dw,
    uw,
    ow,
    ow_pad,
    down_vec,
    up_vec,
    t_ref,
    in_b,
    out_b,
    dg_ref,
    db_ref,
    ug_ref,
    ub_ref,
    local_sem,
    send_sem,
    recv_sem,
    ready_sem,
):
    members, slots, cols, packed = t_ref.shape
    _, _, sub, lanes = comb.shape
    halves = sub // members
    chan = lanes // LANES_OF_LEVELS
    short = chan - TILE
    tiles = lanes // TILE
    total = slots + 2 * HALO
    half_cols = cols // 2
    inner = slots // 2
    mid_lo, mid_hi = HALO, slots // 2
    lat = lax.axis_index("lat")
    lon = lax.axis_index("lon")
    east = {"lat": lat, "lon": lax.rem(lon + 1, n_lon)}
    west = {"lat": lat, "lon": lax.rem(lon + n_lon - 1, n_lon)}
    above = {"lat": jnp.maximum(lat - 1, 0), "lon": lon}
    below = {"lat": jnp.minimum(lat + 1, n_lat - 1), "lon": lon}
    has_above = lat > 0
    has_below = lat < n_lat - 1
    first = lon == 0
    last = lon == n_lon - 1
    before_last = lon == n_lon - 2

    spans = [(0, mid_lo), (mid_hi, slots), (mid_lo, mid_hi)]
    token_loads = []
    for i, (lo, hi) in enumerate(spans):
        span = pl.ds(lo, hi - lo)
        token_loads.append(pltpu.make_async_copy(t_hbm.at[:, span], t_ref.at[:, span], local_sem.at[i]))
        token_loads[i].start()

    barrier = pltpu.get_barrier_semaphore()

    @pl.when(first | last)
    def _():
        pl.semaphore_signal(barrier, inc=1, device_id=west, device_id_type=MESH)

    @pl.when(jnp.logical_not(last))
    def _():
        pl.semaphore_signal(barrier, inc=1, device_id=east, device_id_type=MESH)

    @pl.when(has_below)
    def _():
        pl.semaphore_signal(barrier, inc=1, device_id=below, device_id_type=MESH)

    pairs = [
        (in_b_hbm, in_b),
        (out_b_hbm, out_b),
        (ow_hbm, ow),
        (dg_hbm, dg_ref),
        (db_hbm, db_ref),
        (ug_hbm, ug_ref),
        (ub_hbm, ub_ref),
    ]
    loads = [pltpu.make_async_copy(src, dst, local_sem.at[3 + i]) for i, (src, dst) in enumerate(pairs)]
    for load in loads:
        load.start()
    for block in range(2):
        cut = uw_hbm.at[:, pl.ds(block * 2 * chan, 2 * chan)]
        pltpu.make_async_copy(cut, uw.at[block], local_sem.at[3 + len(pairs)]).start()
    for pos, (e, start, size) in enumerate(down_pieces(chan)):
        at = sum(piece[2] for piece in down_pieces(chan)[:pos] if piece[0] == e)
        cut = dw_hbm.at[pl.ds(start, size)]
        pltpu.make_async_copy(cut, dw.at[e, pl.ds(at, size)], local_sem.at[4 + len(pairs)]).start()

    def take_rows(lo, hi):
        for r in range(lo, hi):
            for member in range(members):
                row = t_ref[member, r].astype(F32)
                for half in range(halves):
                    at = (half * members + member) * cols
                    for t in range(tiles):
                        lane = half * lanes + t * TILE
                        turn_in[r, t, at : at + cols, :] = row[:, lane : lane + TILE]
        for x in range(cols):
            for r in range(lo, hi):
                for t in range(tiles):
                    comb[1 + x, HALO + r, :, t * TILE : (t + 1) * TILE] = turn_in[
                        r, t, pl.ds(x, sub, stride=cols), :
                    ].astype(BF16)

    heard = has_above.astype(jnp.int32) + jnp.logical_not(first).astype(jnp.int32)
    heard = heard + last.astype(jnp.int32) + before_last.astype(jnp.int32)
    @pl.when(heard > 0)
    def _():
        pl.semaphore_wait(barrier, heard)

    @pl.when(jnp.logical_not(first | last))
    def _():
        pl.semaphore_signal(ready_sem.at[0], inc=1, device_id=west, device_id_type=MESH)

    @pl.when(last)
    def _():
        pl.semaphore_signal(ready_sem.at[2], inc=1, device_id=east, device_id_type=MESH)

    @pl.when(has_above)
    def _():
        pl.semaphore_signal(ready_sem.at[1], inc=1, device_id=above, device_id_type=MESH)

    with jax.named_scope("w_tok"):
        token_loads[0].wait()
    take_rows(*spans[0])

    def remote(src, dst, slot, device, landing=None):
        return pltpu.make_async_remote_copy(
            src_ref=src,
            dst_ref=dst,
            send_sem=send_sem.at[slot],
            recv_sem=recv_sem.at[slot if landing is None else landing],
            device_id=device,
            device_id_type=MESH,
        )

    def column(side, x, i, device):
        lo, hi = spans[i]
        span = pl.ds(lo, hi - lo)
        return remote(comb.at[x, pl.ds(HALO + lo, hi - lo)], land.at[side, span], side, device, 3 * side + i)

    to_east = [column(WEST, cols, i, east) for i in range(3)]
    to_west = [column(EAST, 1, i, west) for i in range(3)]
    up = remote(comb.at[pl.ds(1, cols), pl.ds(HALO, HALO)], bot_in, 2, above, 6)
    down = remote(tail, top_in, 3, below, 7)

    def up_side(side):
        return remote(land.at[side, pl.ds(0, HALO)], bot_side.at[side], 4 + side, above, 8 + side)

    def down_side(side):
        return remote(tail_side.at[side], top_side.at[side], 6 + side, below, 10 + side)

    cross_lo = has_above & (lax.rem(lat, 2) == 0)
    cross_hi = has_below & (lax.rem(lat, 2) == 1)

    def sends_cross(side):
        return jnp.where(side == WEST, lon != n_lon - 2, lon != 1)

    def takes_cross(side):
        return jnp.where(side == WEST, jnp.logical_not(last), jnp.logical_not(first))

    def cross(side, x, device, held, landed, slot):
        return pltpu.make_async_remote_copy(
            src_ref=held.at[x],
            dst_ref=landed.at[side],
            send_sem=send_sem.at[8 + side],
            recv_sem=recv_sem.at[slot + side],
            device_id=device,
            device_id_type=MESH,
        )

    def start_early(i):
        @pl.when(before_last)
        def _():
            to_east[i].start()

        @pl.when(jnp.logical_not(first))
        def _():
            to_west[i].start()

    start_early(0)

    @pl.when(has_above)
    def _():
        up.start()

    token_loads[1].wait()
    take_rows(*spans[1])
    start_early(1)
    token_loads[2].wait()
    take_rows(*spans[2])
    start_early(2)

    loads[0].wait()
    loads[1].wait()
    start_in = in_b[lat]
    count = in_b[lat + 1] - start_in
    shift = 2 * out_b[lat] - start_in
    past = count - shift + 2 * TOP
    edge = past // 2
    places[0] = count
    places[1] = shift
    places[2] = edge
    places[3] = out_b[lat + 1] - out_b[lat]
    for x in range(cols):
        for i in range(HALO):
            tail[x, i] = comb[1 + x, count + i]

    with jax.named_scope("w_ready"):

        @pl.when(jnp.logical_not(last | before_last))
        def _():
            pl.semaphore_wait(ready_sem.at[0], 1)
            for copy in to_east:
                copy.start()

    @pl.when(has_below)
    def _():
        pl.semaphore_wait(ready_sem.at[1], 1)
        down.start()

    for load in loads[2:]:
        load.wait()
    pltpu.make_async_copy(uw, uw, local_sem.at[3 + len(pairs)]).wait()
    pltpu.make_async_copy(dw, dw, local_sem.at[4 + len(pairs)]).wait()

    @pl.when(last)
    def _():
        for copy in to_east:
            copy.start()

    for e in range(2):
        for row, ref in ((0, dg_ref), (1, db_ref)):
            vec = ref[...][None]
            cuts = [vec[:, at : at + size] for which, at, size in down_pieces(chan) if which == e]
            down_vec[2 * e + row : 2 * e + row + 1, :] = jnp.concatenate(cuts, axis=1)
    for row, ref in ((0, ug_ref), (1, ub_ref)):
        vec = ref[...][None]
        up_vec[row : row + 1, :] = jnp.concatenate([vec, vec], axis=1)
    ow_pad[...] = jnp.zeros(ow_pad.shape, BF16)
    plain = ow[...]
    moved = jnp.concatenate([jnp.zeros((chan, short), BF16), plain], axis=1)
    for a in range(2):
        ow_pad[0, a, a * short : a * short + chan, 0:chan] = plain
        ow_pad[1, a, a * short : a * short + chan, :] = moved

    turn_fine[2 * (TOP + inner + BOTTOM)] = jnp.zeros(turn_fine.shape[1:], F32)
    turn_merged[inner + BOTTOM] = jnp.zeros(turn_merged.shape[1:], F32)

    def place(r):
        inside = jnp.maximum(r + shift - 1, 0)
        outside = jnp.minimum(HALO + slots + r - past, total - 1)
        return jnp.where(r < past, inside, outside)

    top_rows = [([place(2 * m + a) for a in range(2)], 2 * m, None) for m in range(TOP)]
    inner_rows = [([2 * m + a + shift - 1 for a in range(2)], 2 * m, m - TOP) for m in range(TOP, TOP + inner)]
    bottom_rows = [
        ([place(2 * (edge + i) + a) for a in range(2)], 2 * (TOP + inner + i), inner + i) for i in range(BOTTOM)
    ]
    step = PAIRS * sub

    def first_norm(cells, at=0):
        for i, (col, _, (spots, _, _)) in enumerate(cells):
            blocks = []
            for c in range(2):
                for a in range(2):
                    row = comb[col + c, spots[a]].astype(F32)
                    both = [row[:, p * 2 * chan : (p + 1) * 2 * chan] for p in range(PAIRS)]
                    blocks.append(thirds(jnp.concatenate(both, axis=0)))
            low, done = pair_norm(blocks, 4 * chan)
            even, odd = [v[0] for v in done], [v[2] for v in done]
            for b in (0, 2):
                swapped = pltpu.roll(done[b + 1][1], TILE // 2, 1)
                even.append(jnp.where(low, done[b][1], swapped))
                odd.append(jnp.where(low, swapped, done[b][1]))
            for e, values in ((0, even), (1, odd)):
                for t, value in enumerate(values):
                    lane = slice(t * TILE, (t + 1) * TILE)
                    value = value * down_vec[2 * e : 2 * e + 1, lane] + down_vec[2 * e + 1 : 2 * e + 2, lane]
                    nrm[e, pl.ds(pl.multiple_of((at + i) * step, step), step), lane] = value.astype(BF16)

    def products(cells, ups, skip=0):
        size = len(cells) * step
        whole = len(ups) * size

        def down(e):
            wide = jnp.dot(nrm[e, 0:size, :], dw[e], preferred_element_type=F32)
            coarse[e * size : (e + 1) * size, :] = wide.astype(BF16)
            for i, (_, merged_col, (_, _, merged_at)) in enumerate(cells):
                if merged_col is None or merged_at is None:
                    continue
                for p in range(PAIRS):
                    at = i * step + p * sub
                    for t in range(3):
                        turn_merged[
                            merged_at + skip, (2 * p + e) * 3 + t, pl.ds(merged_col, sub, stride=half_cols), :
                        ] = wide[at : at + sub, t * TILE : (t + 1) * TILE]

        def widen(block, off, which):
            rows = slice(which[0] * size, (which[-1] + 1) * size)
            spread = jnp.dot(coarse[rows, :], uw[block], preferred_element_type=F32)
            for e in which:
                for at in range(0, size, step):
                    lo = (e - which[0]) * size + at
                    _, done = pair_norm([thirds(spread[lo : lo + step])], chan)
                    for t, value in enumerate(done[0]):
                        lane = slice(t * TILE, (t + 1) * TILE)
                        value = value * up_vec[0:1, lane] + up_vec[1:2, lane]
                        to = e * whole + off + at
                        renorm[to : to + step, lane] = value.astype(BF16)

        for which in PARITIES:
            for e in which:
                down(e)
            for u, (block, _) in enumerate(ups):
                widen(block, u * size, which)
        for a in range(2):
            two = [
                jnp.dot(
                    renorm[e * whole : (e + 1) * whole, a * TILE : (a + 2) * TILE],
                    ow_pad[e, a],
                    preferred_element_type=F32,
                )
                for e in range(2)
            ]
            for u, (_, x) in enumerate(ups):
                for i, (_, _, (_, fine_at, _)) in enumerate(cells):
                    for p in range(PAIRS):
                        at = u * size + i * step + p * sub
                        span = slice(at, at + sub)
                        trio = (
                            two[0][span, 0:TILE],
                            two[0][span, TILE : 2 * TILE] + two[1][span, 0:TILE],
                            two[1][span, TILE : 2 * TILE],
                        )
                        for t, value in enumerate(trio):
                            turn_fine[fine_at + a, 3 * p + t, pl.ds(x, sub, stride=cols), :] = value

    own_ups = [(0, 1), (1, 2)]

    def compute_own(rows):
        cells = [(2, 1, row) for row in rows]
        first_norm(cells)
        products(cells, own_ups)

    own = pl.ds(1, cols)

    with jax.named_scope("n_own"):
        first_norm([(2, 1, row) for row in inner_rows])

    with jax.named_scope("c_own"):
        products([(2, 1, row) for row in inner_rows], own_ups)

    with jax.named_scope("w_halo"):

        @pl.when(has_above)
        def _():
            down.wait_recv()

        @pl.when(has_below)
        def _():
            up.wait_recv()
            comb[own, HALO + slots : total] = bot_in[...]

        @pl.when(jnp.logical_not(has_below))
        def _():
            comb[:, HALO + slots : total] = jnp.zeros((cols + 2, HALO, sub, lanes), BF16)

        @pl.when(has_above)
        def _():
            comb[own, 0:HALO] = top_in[...]

        @pl.when(jnp.logical_not(has_above))
        def _():
            comb[:, 0:HALO] = jnp.zeros((cols + 2, HALO, sub, lanes), BF16)

    def start_wrap():
        for copy in to_west:
            copy.start()

    with jax.named_scope("w_wrap"):

        @pl.when(first)
        def _():
            pl.semaphore_wait(ready_sem.at[2], 1)

        @pl.when(first & (lat < n_lat // 2))
        def _():
            start_wrap()

    for side, x, device in ((WEST, cols - 1, east), (EAST, 0, west)):

        @pl.when(cross_lo & sends_cross(side))
        def _():
            cross(side, x, device, top_in, top_side, 10).start()

        @pl.when(cross_hi & sends_cross(side))
        def _():
            cross(side, x, device, bot_in, bot_side, 8).start()

    outer = top_rows + bottom_rows
    with jax.named_scope("c_own_outer"):
        compute_own(outer)

    odd = lax.rem(lon, 2) == 1
    side_one = jnp.where(first | (odd & jnp.logical_not(last)), EAST, WEST)
    side_two = 1 - side_one

    def spared(side):
        return takes_cross(side) & cross_lo, takes_cross(side) & cross_hi

    def arrive(side):
        x = side * (cols + 1)
        for i in range(2):
            lo, hi = spans[i]
            column(side, cols, i, east).wait_recv()
            comb[x, HALO + lo : HALO + hi] = land[side, lo:hi]
        for i in range(HALO):
            tail_side[side, i] = comb[x, count + i]

        lo_spared, hi_spared = spared(side)

        @pl.when(has_above & jnp.logical_not(lo_spared))
        def _():
            up_side(side).start()

        @pl.when(has_below & jnp.logical_not(hi_spared))
        def _():
            down_side(side).start()

    def arrive_rest(side):
        x = side * (cols + 1)
        lo, hi = spans[2]
        column(side, cols, 2, east).wait_recv()
        comb[x, HALO + lo : HALO + hi] = land[side, lo:hi]

    def corner(side):
        x = side * (cols + 1)

        @pl.when(has_above)
        def _():
            down_side(side).wait_recv()
            comb[x, 0:HALO] = top_side[side]

        @pl.when(has_below)
        def _():
            up_side(side).wait_recv()
            comb[x, HALO + slots : total] = bot_side[side]

    def ready(row):
        _, fine_at, _ = row
        return fine_at - 2 * TOP >= mid_hi

    early = [row for row in inner_rows if ready(row)]
    late = [row for row in inner_rows if not ready(row)]
    side_rows = early + late + outer
    assert len(late) == len(outer)

    def place_of(rows):
        return [row[1] for row in side_rows].index(rows[0][1])

    def norm_side(side, rows):
        first_norm([(side * cols, 0, row) for row in rows], place_of(rows))

    def finish_side(side):
        cells = [(side * cols, 0, row) for row in side_rows]
        products(cells, [(1 - side, side * (cols - 1))], side * (inner + BOTTOM + 1))

    hasty = first & (lax.rem(lat, 2) == 1)
    with jax.named_scope("w_one"):
        arrive(side_one)
        arrive_rest(side_one)
    with jax.named_scope("n_one"):
        norm_side(side_one, early)
        norm_side(side_one, late)
    @pl.when(first & (lat >= n_lat // 2))
    def _():
        start_wrap()

    with jax.named_scope("w_hasty"):

        @pl.when(hasty)
        def _():
            arrive(side_two)

    with jax.named_scope("k_one"):
        corner(side_one)
    with jax.named_scope("c_one"):
        norm_side(side_one, outer)
        finish_side(side_one)
    with jax.named_scope("w_two"):

        @pl.when(jnp.logical_not(hasty))
        def _():
            arrive(side_two)

    with jax.named_scope("n_two"):
        norm_side(side_two, early)

    def chosen(own, other):
        spots = [[jnp.where(hasty, x, y) for x, y in zip(a[0], b[0])] for a, b in zip(own, other)]
        at = jnp.where(hasty, place_of(own), place_of(other))
        first_norm([(side_two * cols, 0, (spot, None, None)) for spot in spots], at)

    @pl.when(hasty)
    def _():
        arrive_rest(side_two)

    @pl.when(jnp.logical_not(hasty))
    def _():
        with jax.named_scope("k_two"):
            corner(side_two)

    with jax.named_scope("m_two"):
        chosen(late, outer)

    @pl.when(hasty)
    def _():
        with jax.named_scope("kh_two"):
            corner(side_two)

    @pl.when(jnp.logical_not(hasty))
    def _():
        with jax.named_scope("r_two"):
            arrive_rest(side_two)

    with jax.named_scope("c_two"):
        chosen(outer, late)
        finish_side(side_two)

    whole_column = comb.at[1, pl.ds(HALO, slots)]
    for side, device in ((WEST, east), (EAST, west)):
        remote(whole_column, land.at[side], side, device, 3 * side).wait_send()

    @pl.when(has_above)
    def _():
        up.wait_send()

    @pl.when(has_below)
    def _():
        down.wait_send()

    for side, x, device in ((WEST, cols - 1, east), (EAST, 0, west)):
        lo_spared, hi_spared = spared(side)

        @pl.when(has_above & jnp.logical_not(lo_spared))
        def _():
            up_side(side).wait_send()

        @pl.when(has_below & jnp.logical_not(hi_spared))
        def _():
            down_side(side).wait_send()

        @pl.when((cross_lo | cross_hi) & sends_cross(side))
        def _():
            cross(side, x, device, top_in, top_side, 10).wait_send()


def write_out(turn_merged, turn_fine, places, merged_hbm, fine_hbm, merged_buf, fine_buf, sem):
    members, merged_slots, half_cols, _ = merged_buf.shape
    _, slots, cols, packed = fine_buf.shape
    sub = turn_fine.shape[2] // cols
    halves = sub // members
    lanes = packed // halves
    inner = slots // 2
    count, shift, edge, count_out = places[0], places[1], places[2], places[3]
    copies = []

    def put(turn, index, slot, buf, width, span):
        value = turn[index].astype(BF16)
        for half in range(halves):
            for member in range(members):
                at = (half * members + member) * width
                buf[member, slot, :, half * span : (half + 1) * span] = jnp.concatenate(
                    [value[t, at : at + width] for t in range(span // TILE)], axis=1
                )

    def send(buf, hbm, lo, hi):
        span = pl.ds(lo, hi - lo)
        copy = pltpu.make_async_copy(buf.at[:, span], hbm.at[:, span], sem.at[len(copies)])
        copy.start()
        copies.append(copy)

    for lo in range(0, merged_slots, 4):
        hi = min(lo + 4, merged_slots)
        for slot in range(lo, hi):
            m = slot + TOP
            index = jnp.where(m < edge, slot, jnp.minimum(inner + m - edge, inner + BOTTOM - 1))
            index = jnp.where(slot < count_out, index, inner + BOTTOM)
            put(turn_merged, index, slot, merged_buf, half_cols, 2 * lanes)
        send(merged_buf, merged_hbm, lo, hi)
    for lo in range(0, slots, 5):
        hi = min(lo + 5, slots)
        for slot in range(lo, hi):
            r = slot + 2 * TOP - shift
            after = jnp.minimum(2 * (TOP + inner) + r - 2 * edge, 2 * (TOP + inner + BOTTOM) - 1)
            index = jnp.where(r < 2 * edge, r, after)
            index = jnp.where(slot < count, index, 2 * (TOP + inner + BOTTOM))
            put(turn_fine, index, slot, fine_buf, cols, lanes)
        send(fine_buf, fine_hbm, lo, hi)
    for copy in copies:
        copy.wait()


def body(
    tokens,
    in_bounds,
    out_bounds,
    down_gain,
    down_bias,
    down_weight,
    up_weight,
    up_gain,
    up_bias,
    out_weight,
):
    members, slots, cols, packed = tokens.shape
    chan = down_weight.shape[0] // 4
    halves = packed // (chan * LANES_OF_LEVELS)
    lanes = chan * LANES_OF_LEVELS
    sub = halves * members
    merged_slots = slots // 2 + 1
    half_cols = cols // 2
    inner = slots // 2
    edges = TOP + BOTTOM
    total = slots + 2 * HALO
    most = (inner + edges) * PAIRS * sub
    wide = max(2 * inner, inner + edges) * PAIRS * sub
    n_lat = lax.axis_size("lat")
    n_lon = lax.axis_size("lon")
    vmem = pl.BlockSpec(memory_space=pltpu.VMEM)
    smem = pl.BlockSpec(memory_space=pltpu.SMEM)
    hbm = pl.BlockSpec(memory_space=pltpu.HBM)
    patch = pltpu.VMEM((cols, HALO, sub, lanes), BF16)
    corner = pltpu.VMEM((2, HALO, sub, lanes), BF16)
    operands = (
        in_bounds,
        out_bounds,
        tokens,
        down_weight,
        up_weight,
        out_weight,
        down_gain,
        down_bias,
        up_gain,
        up_bias,
    )
    merged_shape = (members, merged_slots, half_cols, 2 * packed)
    held = pl.pallas_call(
        functools.partial(kernel, n_lat, n_lon),
        out_shape=(
            pltpu.VMEM((2 * (inner + BOTTOM) + 1, 2 * lanes // TILE, half_cols * sub, TILE), F32),
            pltpu.VMEM((2 * (TOP + inner + BOTTOM) + 1, lanes // TILE, cols * sub, TILE), F32),
            pltpu.SMEM((4,), jnp.int32),
        ),
        in_specs=[hbm] * 10,
        out_specs=(vmem, vmem, smem),
        scratch_shapes=[
            pltpu.VMEM((cols + 2, total, sub, lanes), BF16),
            pltpu.VMEM((2, slots, sub, lanes), BF16),
            patch,
            patch,
            corner,
            corner,
            patch,
            corner,
            pltpu.VMEM((2, most, 4 * chan), BF16),
            pltpu.VMEM((2 * most, 2 * chan), BF16),
            pltpu.VMEM((2 * wide, 2 * chan), BF16),
            pltpu.VMEM((slots, lanes // TILE, sub * cols, TILE), F32),
            pltpu.VMEM((2, *down_weight.shape), BF16),
            pltpu.VMEM((2, 2 * chan, 2 * chan), BF16),
            pltpu.VMEM(out_weight.shape, BF16),
            pltpu.VMEM((2, 2, 2 * TILE, 2 * TILE), BF16),
            pltpu.VMEM((4, 4 * chan), F32),
            pltpu.VMEM((2, 2 * chan), F32),
            pltpu.VMEM(tokens.shape, BF16),
            pltpu.SMEM(in_bounds.shape, jnp.int32),
            pltpu.SMEM(out_bounds.shape, jnp.int32),
            pltpu.VMEM(down_gain.shape, F32),
            pltpu.VMEM(down_bias.shape, F32),
            pltpu.VMEM(up_gain.shape, F32),
            pltpu.VMEM(up_bias.shape, F32),
            pltpu.SemaphoreType.DMA((13,)),
            pltpu.SemaphoreType.DMA((10,)),
            pltpu.SemaphoreType.DMA((12,)),
            pltpu.SemaphoreType.REGULAR((3,)),
        ],
        compiler_params=pltpu.CompilerParams(
            collective_id=0, has_side_effects=True, vmem_limit_bytes=48 * 2**20
        ),
    )(*[pltpu.with_memory_space_constraint(x, pltpu.HBM) for x in operands])
    spaces = (pltpu.VMEM, pltpu.VMEM, pltpu.SMEM)
    return pl.pallas_call(
        write_out,
        out_shape=(
            jax.ShapeDtypeStruct(merged_shape, BF16),
            jax.ShapeDtypeStruct(tokens.shape, BF16),
        ),
        in_specs=[vmem, vmem, smem],
        out_specs=(hbm, hbm),
        scratch_shapes=[
            pltpu.VMEM(merged_shape, BF16),
            pltpu.VMEM(tokens.shape, BF16),
            pltpu.SemaphoreType.DMA((pl.cdiv(merged_slots, 4) + pl.cdiv(slots, 5),)),
        ],
        compiler_params=pltpu.CompilerParams(vmem_limit_bytes=48 * 2**20),
    )(*[pltpu.with_memory_space_constraint(x, space) for x, space in zip(held, spaces)])


def solution(mesh):
    return jax.shard_map(
        body,
        mesh=mesh,
        in_specs=(P(None, "lat", "lon", None), P(), P(), P(), P(), P(), P(), P(), P(), P()),
        out_specs=(P(None, "lat", "lon", None), P(None, "lat", "lon", None)),
        check_vma=False,
    )
```

```python
import functools

import jax
import jax.numpy as jnp
from jax import lax
from jax.experimental import pallas as pl
from jax.experimental.pallas import tpu as pltpu
from jax.sharding import PartitionSpec as P

HALO = 3
LANES_OF_LEVELS = 4
PAIRS = LANES_OF_LEVELS // 2
TILE = 128
TOP = 2
BOTTOM = 2
WEST, EAST = 0, 1
MESH = pl.DeviceIdType.MESH
F32 = jnp.float32
BF16 = jnp.bfloat16
PARITIES = ((0, 1),)


def pair_norm(blocks, size):
    low = lax.broadcasted_iota(jnp.int32, blocks[0][0].shape, 1) < TILE // 2
    inv = 1.0 / size

    def totals(tiles):
        one, mid, two = [functools.reduce(jnp.add, group) for group in zip(*tiles)]
        first = jnp.sum(one + jnp.where(low, mid, 0.0), axis=1, keepdims=True) * inv
        second = jnp.sum(two + jnp.where(low, 0.0, mid), axis=1, keepdims=True) * inv
        return first, second

    first, second = totals(blocks)
    mid = jnp.where(low, first, second)
    off = [(one - first, both - mid, two - second) for one, both, two in blocks]
    first, second = totals([tuple(v * v for v in tiles) for tiles in off])
    first, second = lax.rsqrt(first + 1e-05), lax.rsqrt(second + 1e-05)
    mid = jnp.where(low, first, second)
    return low, [(one * first, both * mid, two * second) for one, both, two in off]


def thirds(value):
    return tuple(value[:, t * TILE : (t + 1) * TILE] for t in range(3))


def down_pieces(chan):
    short = chan - TILE
    even = [(0, b * chan, TILE) for b in range(4)] + [(0, b * chan + TILE, short) for b in range(4)]
    odd = [(1, b * chan + short, TILE) for b in range(4)] + [(1, b * chan, short) for b in (1, 0, 3, 2)]
    return even + odd


def kernel(
    n_lat,
    n_lon,
    in_b_hbm,
    out_b_hbm,
    t_hbm,
    dw_hbm,
    uw_hbm,
    ow_hbm,
    dg_hbm,
    db_hbm,
    ug_hbm,
    ub_hbm,
    turn_merged,
    turn_fine,
    places,
    comb,
    land,
    top_in,
    bot_in,
    top_side,
    bot_side,
    tail,
    tail_side,
    nrm,
    coarse,
    renorm,
    turn_in,
    dw,
    uw,
    ow,
    ow_pad,
    down_vec,
    up_vec,
    t_ref,
    in_b,
    out_b,
    dg_ref,
    db_ref,
    ug_ref,
    ub_ref,
    local_sem,
    send_sem,
    recv_sem,
    ready_sem,
):
    members, slots, cols, packed = t_ref.shape
    _, _, sub, lanes = comb.shape
    halves = sub // members
    chan = lanes // LANES_OF_LEVELS
    short = chan - TILE
    tiles = lanes // TILE
    total = slots + 2 * HALO
    half_cols = cols // 2
    inner = slots // 2 - TOP
    blank = inner + BOTTOM + TOP
    mid_lo, mid_hi = HALO, slots // 2
    lat = lax.axis_index("lat")
    lon = lax.axis_index("lon")
    east = {"lat": lat, "lon": lax.rem(lon + 1, n_lon)}
    west = {"lat": lat, "lon": lax.rem(lon + n_lon - 1, n_lon)}
    above = {"lat": jnp.maximum(lat - 1, 0), "lon": lon}
    below = {"lat": jnp.minimum(lat + 1, n_lat - 1), "lon": lon}
    has_above = lat > 0
    has_below = lat < n_lat - 1
    first = lon == 0
    last = lon == n_lon - 1
    before_last = lon == n_lon - 2

    spans = [(0, mid_lo), (mid_hi, slots), (mid_lo, mid_hi)]
    token_loads = []
    for i, (lo, hi) in enumerate(spans):
        span = pl.ds(lo, hi - lo)
        token_loads.append(pltpu.make_async_copy(t_hbm.at[:, span], t_ref.at[:, span], local_sem.at[i]))
        token_loads[i].start()

    barrier = pltpu.get_barrier_semaphore()

    @pl.when(first | last)
    def _():
        pl.semaphore_signal(barrier, inc=1, device_id=west, device_id_type=MESH)

    @pl.when(jnp.logical_not(last))
    def _():
        pl.semaphore_signal(barrier, inc=1, device_id=east, device_id_type=MESH)

    @pl.when(has_below)
    def _():
        pl.semaphore_signal(barrier, inc=1, device_id=below, device_id_type=MESH)

    pairs = [
        (in_b_hbm, in_b),
        (out_b_hbm, out_b),
        (ow_hbm, ow),
        (dg_hbm, dg_ref),
        (db_hbm, db_ref),
        (ug_hbm, ug_ref),
        (ub_hbm, ub_ref),
    ]
    loads = [pltpu.make_async_copy(src, dst, local_sem.at[3 + i]) for i, (src, dst) in enumerate(pairs)]
    for load in loads:
        load.start()
    for block in range(2):
        cut = uw_hbm.at[:, pl.ds(block * 2 * chan, 2 * chan)]
        pltpu.make_async_copy(cut, uw.at[block], local_sem.at[3 + len(pairs)]).start()
    for pos, (e, start, size) in enumerate(down_pieces(chan)):
        at = sum(piece[2] for piece in down_pieces(chan)[:pos] if piece[0] == e)
        cut = dw_hbm.at[pl.ds(start, size)]
        pltpu.make_async_copy(cut, dw.at[e, pl.ds(at, size)], local_sem.at[4 + len(pairs)]).start()

    def take_rows(lo, hi):
        for r in range(lo, hi):
            for member in range(members):
                row = t_ref[member, r].astype(F32)
                for half in range(halves):
                    at = (half * members + member) * cols
                    for t in range(tiles):
                        lane = half * lanes + t * TILE
                        turn_in[r, t, at : at + cols, :] = row[:, lane : lane + TILE]
        for x in range(cols):
            for r in range(lo, hi):
                for t in range(tiles):
                    comb[1 + x, HALO + r, :, t * TILE : (t + 1) * TILE] = turn_in[
                        r, t, pl.ds(x, sub, stride=cols), :
                    ].astype(BF16)

    heard = has_above.astype(jnp.int32) + jnp.logical_not(first).astype(jnp.int32)
    heard = heard + last.astype(jnp.int32) + before_last.astype(jnp.int32)
    @pl.when(heard > 0)
    def _():
        pl.semaphore_wait(barrier, heard)

    @pl.when(jnp.logical_not(first | last))
    def _():
        pl.semaphore_signal(ready_sem.at[0], inc=1, device_id=west, device_id_type=MESH)

    @pl.when(last)
    def _():
        pl.semaphore_signal(ready_sem.at[2], inc=1, device_id=east, device_id_type=MESH)

    @pl.when(has_above)
    def _():
        pl.semaphore_signal(ready_sem.at[1], inc=1, device_id=above, device_id_type=MESH)

    with jax.named_scope("w_tok"):
        token_loads[0].wait()
    take_rows(*spans[0])

    def remote(src, dst, slot, device, landing=None):
        return pltpu.make_async_remote_copy(
            src_ref=src,
            dst_ref=dst,
            send_sem=send_sem.at[slot],
            recv_sem=recv_sem.at[slot if landing is None else landing],
            device_id=device,
            device_id_type=MESH,
        )

    def column(side, x, i, device):
        lo, hi = spans[i]
        span = pl.ds(lo, hi - lo)
        return remote(comb.at[x, pl.ds(HALO + lo, hi - lo)], land.at[side, span], side, device, 3 * side + i)

    to_east = [column(WEST, cols, i, east) for i in range(3)]
    to_west = [column(EAST, 1, i, west) for i in range(3)]
    up = remote(comb.at[pl.ds(1, cols), pl.ds(HALO, HALO)], bot_in, 2, above, 6)
    down = remote(tail, top_in, 3, below, 7)

    def up_side(side):
        return remote(land.at[side, pl.ds(0, HALO)], bot_side.at[side], 4 + side, above, 8 + side)

    def down_side(side):
        return remote(tail_side.at[side], top_side.at[side], 6 + side, below, 10 + side)

    cross_lo = has_above & (lax.rem(lat, 2) == 0)
    cross_hi = has_below & (lax.rem(lat, 2) == 1)

    def sends_cross(side):
        return jnp.where(side == WEST, lon != n_lon - 2, lon != 1)

    def takes_cross(side):
        return jnp.where(side == WEST, jnp.logical_not(last), jnp.logical_not(first))

    def cross(side, x, device, held, landed, slot):
        return pltpu.make_async_remote_copy(
            src_ref=held.at[x],
            dst_ref=landed.at[side],
            send_sem=send_sem.at[8 + side],
            recv_sem=recv_sem.at[slot + side],
            device_id=device,
            device_id_type=MESH,
        )

    def start_early(i):
        @pl.when(before_last)
        def _():
            to_east[i].start()

        @pl.when(jnp.logical_not(first))
        def _():
            to_west[i].start()

    start_early(0)

    @pl.when(has_above)
    def _():
        up.start()

    token_loads[1].wait()
    take_rows(*spans[1])
    start_early(1)
    token_loads[2].wait()
    take_rows(*spans[2])
    start_early(2)

    loads[0].wait()
    loads[1].wait()
    start_in = in_b[lat]
    count = in_b[lat + 1] - start_in
    shift = 2 * out_b[lat] - start_in
    past = count - shift + 2 * TOP
    edge = past // 2
    places[0] = count
    places[1] = shift
    places[2] = edge
    places[3] = out_b[lat + 1] - out_b[lat]
    for x in range(cols):
        for i in range(HALO):
            tail[x, i] = comb[1 + x, count + i]

    with jax.named_scope("w_ready"):

        @pl.when(jnp.logical_not(last | before_last))
        def _():
            pl.semaphore_wait(ready_sem.at[0], 1)
            for copy in to_east:
                copy.start()

    @pl.when(has_below)
    def _():
        pl.semaphore_wait(ready_sem.at[1], 1)
        down.start()

    for load in loads[2:]:
        load.wait()
    pltpu.make_async_copy(uw, uw, local_sem.at[3 + len(pairs)]).wait()
    pltpu.make_async_copy(dw, dw, local_sem.at[4 + len(pairs)]).wait()

    @pl.when(last)
    def _():
        for copy in to_east:
            copy.start()

    for e in range(2):
        for row, ref in ((0, dg_ref), (1, db_ref)):
            vec = ref[...][None]
            cuts = [vec[:, at : at + size] for which, at, size in down_pieces(chan) if which == e]
            down_vec[2 * e + row : 2 * e + row + 1, :] = jnp.concatenate(cuts, axis=1)
    for row, ref in ((0, ug_ref), (1, ub_ref)):
        vec = ref[...][None]
        up_vec[row : row + 1, :] = jnp.concatenate([vec, vec], axis=1)
    ow_pad[...] = jnp.zeros(ow_pad.shape, BF16)
    plain = ow[...]
    moved = jnp.concatenate([jnp.zeros((chan, short), BF16), plain], axis=1)
    for a in range(2):
        ow_pad[0, a, a * short : a * short + chan, 0:chan] = plain
        ow_pad[1, a, a * short : a * short + chan, :] = moved

    turn_fine[2 * (TOP + inner + BOTTOM)] = jnp.zeros(turn_fine.shape[1:], F32)
    turn_merged[blank] = jnp.zeros(turn_merged.shape[1:], F32)

    def place(r):
        inside = jnp.maximum(r + shift - 1, 0)
        outside = jnp.minimum(HALO + slots + r - past, total - 1)
        return jnp.where(r < past, inside, outside)

    def own_place(r):
        return r + shift - 1

    top_rows = []
    for m, instead in ((0, shift < HALO), (1, shift == 0)):
        spots = [jnp.where(instead, own_place(2 * (TOP + inner + m) + a), place(2 * m + a)) for a in range(2)]
        top_rows.append((spots, 2 * m, inner + BOTTOM + m))
    inner_rows = [([own_place(2 * m + a) for a in range(2)], 2 * m, m - TOP) for m in range(TOP, TOP + inner)]
    bottom_rows = [
        ([place(2 * (edge + i) + a) for a in range(2)], 2 * (TOP + inner + i), inner + i) for i in range(BOTTOM)
    ]
    step = PAIRS * sub

    def first_norm(cells, at=0):
        for i, (col, _, (spots, _, _)) in enumerate(cells):
            blocks = []
            for c in range(2):
                for a in range(2):
                    row = comb[col + c, spots[a]].astype(F32)
                    both = [row[:, p * 2 * chan : (p + 1) * 2 * chan] for p in range(PAIRS)]
                    blocks.append(thirds(jnp.concatenate(both, axis=0)))
            low, done = pair_norm(blocks, 4 * chan)
            even, odd = [v[0] for v in done], [v[2] for v in done]
            for b in (0, 2):
                swapped = pltpu.roll(done[b + 1][1], TILE // 2, 1)
                even.append(jnp.where(low, done[b][1], swapped))
                odd.append(jnp.where(low, swapped, done[b][1]))
            for e, values in ((0, even), (1, odd)):
                for t, value in enumerate(values):
                    lane = slice(t * TILE, (t + 1) * TILE)
                    value = value * down_vec[2 * e : 2 * e + 1, lane] + down_vec[2 * e + 1 : 2 * e + 2, lane]
                    nrm[e, pl.ds(pl.multiple_of((at + i) * step, step), step), lane] = value.astype(BF16)

    def products(cells, ups, skip=0):
        size = len(cells) * step
        whole = len(ups) * size

        def down(e):
            wide = jnp.dot(nrm[e, 0:size, :], dw[e], preferred_element_type=F32)
            coarse[e * size : (e + 1) * size, :] = wide.astype(BF16)
            for i, (_, merged_col, (_, _, merged_at)) in enumerate(cells):
                if merged_col is None or merged_at is None:
                    continue
                for p in range(PAIRS):
                    at = i * step + p * sub
                    for t in range(3):
                        turn_merged[
                            merged_at + skip, (2 * p + e) * 3 + t, pl.ds(merged_col, sub, stride=half_cols), :
                        ] = wide[at : at + sub, t * TILE : (t + 1) * TILE]

        def widen(block, off, which):
            rows = slice(which[0] * size, (which[-1] + 1) * size)
            spread = jnp.dot(coarse[rows, :], uw[block], preferred_element_type=F32)
            for e in which:
                for at in range(0, size, step):
                    lo = (e - which[0]) * size + at
                    _, done = pair_norm([thirds(spread[lo : lo + step])], chan)
                    for t, value in enumerate(done[0]):
                        lane = slice(t * TILE, (t + 1) * TILE)
                        value = value * up_vec[0:1, lane] + up_vec[1:2, lane]
                        to = e * whole + off + at
                        renorm[to : to + step, lane] = value.astype(BF16)

        for which in PARITIES:
            for e in which:
                down(e)
            for u, (block, _) in enumerate(ups):
                widen(block, u * size, which)
        for a in range(2):
            two = [
                jnp.dot(
                    renorm[e * whole : (e + 1) * whole, a * TILE : (a + 2) * TILE],
                    ow_pad[e, a],
                    preferred_element_type=F32,
                )
                for e in range(2)
            ]
            for u, (_, x) in enumerate(ups):
                for i, (_, _, (_, fine_at, _)) in enumerate(cells):
                    for p in range(PAIRS):
                        at = u * size + i * step + p * sub
                        span = slice(at, at + sub)
                        trio = (
                            two[0][span, 0:TILE],
                            two[0][span, TILE : 2 * TILE] + two[1][span, 0:TILE],
                            two[1][span, TILE : 2 * TILE],
                        )
                        for t, value in enumerate(trio):
                            turn_fine[fine_at + a, 3 * p + t, pl.ds(x, sub, stride=cols), :] = value

    own_ups = [(0, 1), (1, 2)]

    def compute_own(rows):
        cells = [(2, 1, row) for row in rows]
        first_norm(cells)
        products(cells, own_ups)

    own = pl.ds(1, cols)

    with jax.named_scope("n_own"):
        first_norm([(2, 1, row) for row in inner_rows])

    with jax.named_scope("c_own"):
        products([(2, 1, row) for row in inner_rows], own_ups)

    with jax.named_scope("w_halo"):

        @pl.when(has_above)
        def _():
            down.wait_recv()

        @pl.when(has_below)
        def _():
            up.wait_recv()
            comb[own, HALO + slots : total] = bot_in[...]

        @pl.when(jnp.logical_not(has_below))
        def _():
            comb[:, HALO + slots : total] = jnp.zeros((cols + 2, HALO, sub, lanes), BF16)

        @pl.when(has_above)
        def _():
            comb[own, 0:HALO] = top_in[...]

        @pl.when(jnp.logical_not(has_above))
        def _():
            comb[:, 0:HALO] = jnp.zeros((cols + 2, HALO, sub, lanes), BF16)

    def start_wrap():
        for copy in to_west:
            copy.start()

    with jax.named_scope("w_wrap"):

        @pl.when(first)
        def _():
            pl.semaphore_wait(ready_sem.at[2], 1)

        @pl.when(first & (lat < n_lat // 2))
        def _():
            start_wrap()

    for side, x, device in ((WEST, cols - 1, east), (EAST, 0, west)):

        @pl.when(cross_lo & sends_cross(side))
        def _():
            cross(side, x, device, top_in, top_side, 10).start()

        @pl.when(cross_hi & sends_cross(side))
        def _():
            cross(side, x, device, bot_in, bot_side, 8).start()

    outer = top_rows + bottom_rows
    with jax.named_scope("c_own_outer"):
        compute_own(outer)

    odd = lax.rem(lon, 2) == 1
    side_one = jnp.where(first | (odd & jnp.logical_not(last)), EAST, WEST)
    side_two = 1 - side_one

    def spared(side):
        return takes_cross(side) & cross_lo, takes_cross(side) & cross_hi

    def arrive(side):
        x = side * (cols + 1)
        for i in range(2):
            lo, hi = spans[i]
            column(side, cols, i, east).wait_recv()
            comb[x, HALO + lo : HALO + hi] = land[side, lo:hi]
        for i in range(HALO):
            tail_side[side, i] = comb[x, count + i]

        lo_spared, hi_spared = spared(side)

        @pl.when(has_above & jnp.logical_not(lo_spared))
        def _():
            up_side(side).start()

        @pl.when(has_below & jnp.logical_not(hi_spared))
        def _():
            down_side(side).start()

    def arrive_rest(side):
        x = side * (cols + 1)
        lo, hi = spans[2]
        column(side, cols, 2, east).wait_recv()
        comb[x, HALO + lo : HALO + hi] = land[side, lo:hi]

    def corner(side):
        x = side * (cols + 1)

        @pl.when(has_above)
        def _():
            down_side(side).wait_recv()
            comb[x, 0:HALO] = top_side[side]

        @pl.when(has_below)
        def _():
            up_side(side).wait_recv()
            comb[x, HALO + slots : total] = bot_side[side]

    def ready(row):
        _, fine_at, _ = row
        return fine_at - 2 * TOP >= mid_hi

    early = [row for row in inner_rows if ready(row)]
    late = [row for row in inner_rows if not ready(row)]
    side_rows = early + late + outer
    assert len(late) == len(outer)

    def place_of(rows):
        return [row[1] for row in side_rows].index(rows[0][1])

    def norm_side(side, rows):
        first_norm([(side * cols, 0, row) for row in rows], place_of(rows))

    def finish_side(side):
        cells = [(side * cols, 0, row) for row in side_rows]
        products(cells, [(1 - side, side * (cols - 1))], side * (blank + 1))

    hasty = first & (lax.rem(lat, 2) == 1)
    with jax.named_scope("w_one"):
        arrive(side_one)
        arrive_rest(side_one)
    with jax.named_scope("n_one"):
        norm_side(side_one, early)
        norm_side(side_one, late)
    @pl.when(first & (lat >= n_lat // 2))
    def _():
        start_wrap()

    with jax.named_scope("w_hasty"):

        @pl.when(hasty)
        def _():
            arrive(side_two)

    with jax.named_scope("k_one"):
        corner(side_one)
    with jax.named_scope("c_one"):
        norm_side(side_one, outer)
        finish_side(side_one)
    with jax.named_scope("w_two"):

        @pl.when(jnp.logical_not(hasty))
        def _():
            arrive(side_two)

    with jax.named_scope("n_two"):
        norm_side(side_two, early)

    def chosen(own, other):
        spots = [[jnp.where(hasty, x, y) for x, y in zip(a[0], b[0])] for a, b in zip(own, other)]
        at = jnp.where(hasty, place_of(own), place_of(other))
        first_norm([(side_two * cols, 0, (spot, None, None)) for spot in spots], at)

    @pl.when(hasty)
    def _():
        arrive_rest(side_two)

    @pl.when(jnp.logical_not(hasty))
    def _():
        with jax.named_scope("k_two"):
            corner(side_two)

    with jax.named_scope("m_two"):
        chosen(late, outer)

    @pl.when(hasty)
    def _():
        with jax.named_scope("kh_two"):
            corner(side_two)

    @pl.when(jnp.logical_not(hasty))
    def _():
        with jax.named_scope("r_two"):
            arrive_rest(side_two)

    with jax.named_scope("c_two"):
        chosen(outer, late)
        finish_side(side_two)

    whole_column = comb.at[1, pl.ds(HALO, slots)]
    for side, device in ((WEST, east), (EAST, west)):
        remote(whole_column, land.at[side], side, device, 3 * side).wait_send()

    @pl.when(has_above)
    def _():
        up.wait_send()

    @pl.when(has_below)
    def _():
        down.wait_send()

    for side, x, device in ((WEST, cols - 1, east), (EAST, 0, west)):
        lo_spared, hi_spared = spared(side)

        @pl.when(has_above & jnp.logical_not(lo_spared))
        def _():
            up_side(side).wait_send()

        @pl.when(has_below & jnp.logical_not(hi_spared))
        def _():
            down_side(side).wait_send()

        @pl.when((cross_lo | cross_hi) & sends_cross(side))
        def _():
            cross(side, x, device, top_in, top_side, 10).wait_send()


def write_out(turn_merged, turn_fine, places, merged_hbm, fine_hbm, merged_buf, fine_buf, sem):
    members, merged_slots, half_cols, _ = merged_buf.shape
    _, slots, cols, packed = fine_buf.shape
    sub = turn_fine.shape[2] // cols
    halves = sub // members
    lanes = packed // halves
    inner = slots // 2 - TOP
    blank = inner + BOTTOM + TOP
    count, shift, edge, count_out = places[0], places[1], places[2], places[3]
    copies = []

    def put(turn, index, slot, buf, width, span):
        value = turn[index].astype(BF16)
        for half in range(halves):
            for member in range(members):
                at = (half * members + member) * width
                buf[member, slot, :, half * span : (half + 1) * span] = jnp.concatenate(
                    [value[t, at : at + width] for t in range(span // TILE)], axis=1
                )

    def send(buf, hbm, lo, hi):
        span = pl.ds(lo, hi - lo)
        copy = pltpu.make_async_copy(buf.at[:, span], hbm.at[:, span], sem.at[len(copies)])
        copy.start()
        copies.append(copy)

    for lo in range(0, slots, 5):
        hi = min(lo + 5, slots)
        for slot in range(lo, hi):
            r = slot + 2 * TOP - shift
            after = jnp.minimum(2 * (TOP + inner) + r - 2 * edge, 2 * (TOP + inner + BOTTOM) - 1)
            before = jnp.where(r < 2 * (TOP + inner), r, r - 2 * (TOP + inner))
            index = jnp.where(r < 2 * edge, before, after)
            index = jnp.where(slot < count, index, 2 * (TOP + inner + BOTTOM))
            put(turn_fine, index, slot, fine_buf, cols, lanes)
        send(fine_buf, fine_hbm, lo, hi)
    for lo in range(0, merged_slots, 4):
        hi = min(lo + 4, merged_slots)
        for slot in range(lo, hi):
            m = slot + TOP
            index = min(slot if slot < inner else slot + BOTTOM, blank - 1)
            index = jnp.where(m < edge, index, jnp.minimum(inner + m - edge, inner + BOTTOM - 1))
            index = jnp.where(slot < count_out, index, blank)
            put(turn_merged, index, slot, merged_buf, half_cols, 2 * lanes)
        send(merged_buf, merged_hbm, lo, hi)
    for copy in copies:
        copy.wait()


def body(
    tokens,
    in_bounds,
    out_bounds,
    down_gain,
    down_bias,
    down_weight,
    up_weight,
    up_gain,
    up_bias,
    out_weight,
):
    members, slots, cols, packed = tokens.shape
    chan = down_weight.shape[0] // 4
    halves = packed // (chan * LANES_OF_LEVELS)
    lanes = chan * LANES_OF_LEVELS
    sub = halves * members
    merged_slots = slots // 2 + 1
    half_cols = cols // 2
    inner = slots // 2 - TOP
    edges = TOP + BOTTOM
    total = slots + 2 * HALO
    most = (inner + edges) * PAIRS * sub
    wide = max(2 * inner, inner + edges) * PAIRS * sub
    n_lat = lax.axis_size("lat")
    n_lon = lax.axis_size("lon")
    vmem = pl.BlockSpec(memory_space=pltpu.VMEM)
    smem = pl.BlockSpec(memory_space=pltpu.SMEM)
    hbm = pl.BlockSpec(memory_space=pltpu.HBM)
    patch = pltpu.VMEM((cols, HALO, sub, lanes), BF16)
    corner = pltpu.VMEM((2, HALO, sub, lanes), BF16)
    operands = (
        in_bounds,
        out_bounds,
        tokens,
        down_weight,
        up_weight,
        out_weight,
        down_gain,
        down_bias,
        up_gain,
        up_bias,
    )
    merged_shape = (members, merged_slots, half_cols, 2 * packed)
    held = pl.pallas_call(
        functools.partial(kernel, n_lat, n_lon),
        out_shape=(
            pltpu.VMEM((2 * (inner + edges + 1), 2 * lanes // TILE, half_cols * sub, TILE), F32),
            pltpu.VMEM((2 * (TOP + inner + BOTTOM) + 1, lanes // TILE, cols * sub, TILE), F32),
            pltpu.SMEM((4,), jnp.int32),
        ),
        in_specs=[hbm] * 10,
        out_specs=(vmem, vmem, smem),
        scratch_shapes=[
            pltpu.VMEM((cols + 2, total, sub, lanes), BF16),
            pltpu.VMEM((2, slots, sub, lanes), BF16),
            patch,
            patch,
            corner,
            corner,
            patch,
            corner,
            pltpu.VMEM((2, most, 4 * chan), BF16),
            pltpu.VMEM((2 * most, 2 * chan), BF16),
            pltpu.VMEM((2 * wide, 2 * chan), BF16),
            pltpu.VMEM((slots, lanes // TILE, sub * cols, TILE), F32),
            pltpu.VMEM((2, *down_weight.shape), BF16),
            pltpu.VMEM((2, 2 * chan, 2 * chan), BF16),
            pltpu.VMEM(out_weight.shape, BF16),
            pltpu.VMEM((2, 2, 2 * TILE, 2 * TILE), BF16),
            pltpu.VMEM((4, 4 * chan), F32),
            pltpu.VMEM((2, 2 * chan), F32),
            pltpu.VMEM(tokens.shape, BF16),
            pltpu.SMEM(in_bounds.shape, jnp.int32),
            pltpu.SMEM(out_bounds.shape, jnp.int32),
            pltpu.VMEM(down_gain.shape, F32),
            pltpu.VMEM(down_bias.shape, F32),
            pltpu.VMEM(up_gain.shape, F32),
            pltpu.VMEM(up_bias.shape, F32),
            pltpu.SemaphoreType.DMA((13,)),
            pltpu.SemaphoreType.DMA((10,)),
            pltpu.SemaphoreType.DMA((12,)),
            pltpu.SemaphoreType.REGULAR((3,)),
        ],
        compiler_params=pltpu.CompilerParams(
            collective_id=0, has_side_effects=True, vmem_limit_bytes=48 * 2**20
        ),
    )(*[pltpu.with_memory_space_constraint(x, pltpu.HBM) for x in operands])
    spaces = (pltpu.VMEM, pltpu.VMEM, pltpu.SMEM)
    return pl.pallas_call(
        write_out,
        out_shape=(
            jax.ShapeDtypeStruct(merged_shape, BF16),
            jax.ShapeDtypeStruct(tokens.shape, BF16),
        ),
        in_specs=[vmem, vmem, smem],
        out_specs=(hbm, hbm),
        scratch_shapes=[
            pltpu.VMEM(merged_shape, BF16),
            pltpu.VMEM(tokens.shape, BF16),
            pltpu.SemaphoreType.DMA((pl.cdiv(merged_slots, 4) + pl.cdiv(slots, 5),)),
        ],
        compiler_params=pltpu.CompilerParams(vmem_limit_bytes=48 * 2**20),
    )(*[pltpu.with_memory_space_constraint(x, space) for x, space in zip(held, spaces)])


def solution(mesh):
    return jax.shard_map(
        body,
        mesh=mesh,
        in_specs=(P(None, "lat", "lon", None), P(), P(), P(), P(), P(), P(), P(), P(), P()),
        out_specs=(P(None, "lat", "lon", None), P(None, "lat", "lon", None)),
        check_vma=False,
    )
```

```python
import functools

import jax
import jax.numpy as jnp
from jax import lax
from jax.experimental import pallas as pl
from jax.experimental.pallas import tpu as pltpu
from jax.sharding import PartitionSpec as P

HALO = 3
LANES_OF_LEVELS = 4
PAIRS = LANES_OF_LEVELS // 2
TILE = 128
TOP = 2
BOTTOM = 2
WEST, EAST = 0, 1
MESH = pl.DeviceIdType.MESH
F32 = jnp.float32
BF16 = jnp.bfloat16
PARITIES = ((0, 1),)


def pair_norm(blocks, size):
    low = lax.broadcasted_iota(jnp.int32, blocks[0][0].shape, 1) < TILE // 2
    inv = 1.0 / size

    def totals(tiles):
        one, mid, two = [functools.reduce(jnp.add, group) for group in zip(*tiles)]
        first = jnp.sum(one + jnp.where(low, mid, 0.0), axis=1, keepdims=True) * inv
        second = jnp.sum(two + jnp.where(low, 0.0, mid), axis=1, keepdims=True) * inv
        return first, second

    first, second = totals(blocks)
    mid = jnp.where(low, first, second)
    off = [(one - first, both - mid, two - second) for one, both, two in blocks]
    first, second = totals([tuple(v * v for v in tiles) for tiles in off])
    first, second = lax.rsqrt(first + 1e-05), lax.rsqrt(second + 1e-05)
    mid = jnp.where(low, first, second)
    return low, [(one * first, both * mid, two * second) for one, both, two in off]


def thirds(value):
    return tuple(value[:, t * TILE : (t + 1) * TILE] for t in range(3))


def down_pieces(chan):
    short = chan - TILE
    even = [(0, b * chan, TILE) for b in range(4)] + [(0, b * chan + TILE, short) for b in range(4)]
    odd = [(1, b * chan + short, TILE) for b in range(4)] + [(1, b * chan, short) for b in (1, 0, 3, 2)]
    return even + odd


def kernel(
    n_lat,
    n_lon,
    in_b_hbm,
    out_b_hbm,
    t_hbm,
    dw_hbm,
    uw_hbm,
    ow_hbm,
    dg_hbm,
    db_hbm,
    ug_hbm,
    ub_hbm,
    turn_merged,
    turn_fine,
    places,
    comb,
    land,
    top_in,
    bot_in,
    top_side,
    bot_side,
    tail,
    tail_side,
    nrm,
    coarse,
    renorm,
    turn_in,
    dw,
    uw,
    ow,
    ow_pad,
    down_vec,
    up_vec,
    t_ref,
    in_b,
    out_b,
    dg_ref,
    db_ref,
    ug_ref,
    ub_ref,
    local_sem,
    send_sem,
    recv_sem,
    ready_sem,
):
    members, slots, cols, packed = t_ref.shape
    _, _, sub, lanes = comb.shape
    halves = sub // members
    chan = lanes // LANES_OF_LEVELS
    short = chan - TILE
    tiles = lanes // TILE
    total = slots + 2 * HALO
    half_cols = cols // 2
    inner = slots // 2 - TOP
    blank = inner + BOTTOM + TOP
    mid_lo, mid_hi = HALO, slots // 2
    lat = lax.axis_index("lat")
    lon = lax.axis_index("lon")
    east = {"lat": lat, "lon": lax.rem(lon + 1, n_lon)}
    west = {"lat": lat, "lon": lax.rem(lon + n_lon - 1, n_lon)}
    above = {"lat": jnp.maximum(lat - 1, 0), "lon": lon}
    below = {"lat": jnp.minimum(lat + 1, n_lat - 1), "lon": lon}
    has_above = lat > 0
    has_below = lat < n_lat - 1
    first = lon == 0
    last = lon == n_lon - 1
    before_last = lon == n_lon - 2

    spans = [(0, mid_lo), (mid_hi, slots), (mid_lo, mid_hi)]
    token_loads = []
    for i, (lo, hi) in enumerate(spans):
        span = pl.ds(lo, hi - lo)
        token_loads.append(pltpu.make_async_copy(t_hbm.at[:, span], t_ref.at[:, span], local_sem.at[i]))
        token_loads[i].start()

    barrier = pltpu.get_barrier_semaphore()

    @pl.when(first | last)
    def _():
        pl.semaphore_signal(barrier, inc=1, device_id=west, device_id_type=MESH)

    @pl.when(jnp.logical_not(last))
    def _():
        pl.semaphore_signal(barrier, inc=1, device_id=east, device_id_type=MESH)

    @pl.when(has_below)
    def _():
        pl.semaphore_signal(barrier, inc=1, device_id=below, device_id_type=MESH)

    pairs = [
        (in_b_hbm, in_b),
        (out_b_hbm, out_b),
        (ow_hbm, ow),
        (dg_hbm, dg_ref),
        (db_hbm, db_ref),
        (ug_hbm, ug_ref),
        (ub_hbm, ub_ref),
    ]
    free_sems = [send_sem.at[i] for i in (3, 9, 4, 5, 6, 7, 8)]
    loads = [pltpu.make_async_copy(src, dst, sem) for (src, dst), sem in zip(pairs, free_sems)]
    for load in loads:
        load.start()
    for block in range(2):
        cut = uw_hbm.at[:, pl.ds(block * 2 * chan, 2 * chan)]
        pltpu.make_async_copy(cut, uw.at[block], local_sem.at[3]).start()
    for pos, (e, start, size) in enumerate(down_pieces(chan)):
        at = sum(piece[2] for piece in down_pieces(chan)[:pos] if piece[0] == e)
        cut = dw_hbm.at[pl.ds(start, size)]
        pltpu.make_async_copy(cut, dw.at[e, pl.ds(at, size)], local_sem.at[4]).start()

    def take_rows(lo, hi):
        for r in range(lo, hi):
            for member in range(members):
                row = t_ref[member, r].astype(F32)
                for half in range(halves):
                    at = (half * members + member) * cols
                    for t in range(tiles):
                        lane = half * lanes + t * TILE
                        turn_in[r, t, at : at + cols, :] = row[:, lane : lane + TILE]
        for x in range(cols):
            for r in range(lo, hi):
                for t in range(tiles):
                    comb[1 + x, HALO + r, :, t * TILE : (t + 1) * TILE] = turn_in[
                        r, t, pl.ds(x, sub, stride=cols), :
                    ].astype(BF16)

    heard = has_above.astype(jnp.int32) + jnp.logical_not(first).astype(jnp.int32)
    heard = heard + last.astype(jnp.int32) + before_last.astype(jnp.int32)
    @pl.when(heard > 0)
    def _():
        pl.semaphore_wait(barrier, heard)

    @pl.when(jnp.logical_not(first | last))
    def _():
        pl.semaphore_signal(ready_sem.at[0], inc=1, device_id=west, device_id_type=MESH)

    @pl.when(last)
    def _():
        pl.semaphore_signal(ready_sem.at[2], inc=1, device_id=east, device_id_type=MESH)

    @pl.when(has_above)
    def _():
        pl.semaphore_signal(ready_sem.at[1], inc=1, device_id=above, device_id_type=MESH)

    with jax.named_scope("w_tok"):
        token_loads[0].wait()
    take_rows(*spans[0])

    def remote(src, dst, slot, device, landing=None):
        return pltpu.make_async_remote_copy(
            src_ref=src,
            dst_ref=dst,
            send_sem=send_sem.at[slot],
            recv_sem=recv_sem.at[slot if landing is None else landing],
            device_id=device,
            device_id_type=MESH,
        )

    def column(side, x, i, device):
        lo, hi = spans[i]
        span = pl.ds(lo, hi - lo)
        return remote(comb.at[x, pl.ds(HALO + lo, hi - lo)], land.at[side, span], side, device, 3 * side + i)

    to_east = [column(WEST, cols, i, east) for i in range(3)]
    to_west = [column(EAST, 1, i, west) for i in range(3)]
    up = remote(comb.at[pl.ds(1, cols), pl.ds(HALO, HALO)], bot_in, 2, above, 6)
    down = remote(tail, top_in, 3, below, 7)

    def up_side(side):
        return remote(land.at[side, pl.ds(0, HALO)], bot_side.at[side], 4 + side, above, 8 + side)

    def down_side(side):
        return remote(tail_side.at[side], top_side.at[side], 6 + side, below, 10 + side)

    cross_lo = has_above & (lax.rem(lat, 2) == 0)
    cross_hi = has_below & (lax.rem(lat, 2) == 1)

    def sends_cross(side):
        return jnp.where(side == WEST, lon != n_lon - 2, lon != 1)

    def takes_cross(side):
        return jnp.where(side == WEST, jnp.logical_not(last), jnp.logical_not(first))

    def cross(side, x, device, held, landed, slot):
        return pltpu.make_async_remote_copy(
            src_ref=held.at[x],
            dst_ref=landed.at[side],
            send_sem=send_sem.at[8 + side],
            recv_sem=recv_sem.at[slot + side],
            device_id=device,
            device_id_type=MESH,
        )

    def start_early(i):
        @pl.when(before_last)
        def _():
            to_east[i].start()

        @pl.when(jnp.logical_not(first))
        def _():
            to_west[i].start()

    start_early(0)

    @pl.when(has_above)
    def _():
        up.start()

    token_loads[1].wait()
    take_rows(*spans[1])
    start_early(1)
    token_loads[2].wait()
    take_rows(*spans[2])
    start_early(2)

    loads[0].wait()
    loads[1].wait()
    start_in = in_b[lat]
    count = in_b[lat + 1] - start_in
    shift = 2 * out_b[lat] - start_in
    past = count - shift + 2 * TOP
    edge = past // 2
    places[0] = count
    places[1] = shift
    places[2] = edge
    places[3] = out_b[lat + 1] - out_b[lat]
    for x in range(cols):
        for i in range(HALO):
            tail[x, i] = comb[1 + x, count + i]

    with jax.named_scope("w_ready"):

        @pl.when(jnp.logical_not(last | before_last))
        def _():
            pl.semaphore_wait(ready_sem.at[0], 1)
            for copy in to_east:
                copy.start()

    @pl.when(has_below)
    def _():
        pl.semaphore_wait(ready_sem.at[1], 1)
        down.start()

    for load in loads[2:]:
        load.wait()
    pltpu.make_async_copy(uw, uw, local_sem.at[3]).wait()
    pltpu.make_async_copy(dw, dw, local_sem.at[4]).wait()

    @pl.when(last)
    def _():
        for copy in to_east:
            copy.start()

    for e in range(2):
        for row, ref in ((0, dg_ref), (1, db_ref)):
            vec = ref[...][None]
            cuts = [vec[:, at : at + size] for which, at, size in down_pieces(chan) if which == e]
            down_vec[2 * e + row : 2 * e + row + 1, :] = jnp.concatenate(cuts, axis=1)
    for row, ref in ((0, ug_ref), (1, ub_ref)):
        vec = ref[...][None]
        up_vec[row : row + 1, :] = jnp.concatenate([vec, vec], axis=1)
    ow_pad[...] = jnp.zeros(ow_pad.shape, BF16)
    plain = ow[...]
    moved = jnp.concatenate([jnp.zeros((chan, short), BF16), plain], axis=1)
    for a in range(2):
        ow_pad[0, a, a * short : a * short + chan, 0:chan] = plain
        ow_pad[1, a, a * short : a * short + chan, :] = moved

    turn_fine[2 * (TOP + inner + BOTTOM)] = jnp.zeros(turn_fine.shape[1:], F32)
    turn_merged[blank] = jnp.zeros(turn_merged.shape[1:], F32)

    def place(r):
        inside = jnp.maximum(r + shift - 1, 0)
        outside = jnp.minimum(HALO + slots + r - past, total - 1)
        return jnp.where(r < past, inside, outside)

    def own_place(r):
        return r + shift - 1

    top_rows = []
    for m, instead in ((0, shift < HALO), (1, shift == 0)):
        spots = [jnp.where(instead, own_place(2 * (TOP + inner + m) + a), place(2 * m + a)) for a in range(2)]
        top_rows.append((spots, 2 * m, inner + BOTTOM + m))
    inner_rows = [([own_place(2 * m + a) for a in range(2)], 2 * m, m - TOP) for m in range(TOP, TOP + inner)]
    bottom_rows = [
        ([place(2 * (edge + i) + a) for a in range(2)], 2 * (TOP + inner + i), inner + i) for i in range(BOTTOM)
    ]
    step = PAIRS * sub

    def first_norm(cells, at=0):
        for i, (col, _, (spots, _, _)) in enumerate(cells):
            blocks = []
            for c in range(2):
                for a in range(2):
                    row = comb[col + c, spots[a]].astype(F32)
                    both = [row[:, p * 2 * chan : (p + 1) * 2 * chan] for p in range(PAIRS)]
                    blocks.append(thirds(jnp.concatenate(both, axis=0)))
            low, done = pair_norm(blocks, 4 * chan)
            even, odd = [v[0] for v in done], [v[2] for v in done]
            for b in (0, 2):
                swapped = pltpu.roll(done[b + 1][1], TILE // 2, 1)
                even.append(jnp.where(low, done[b][1], swapped))
                odd.append(jnp.where(low, swapped, done[b][1]))
            for e, values in ((0, even), (1, odd)):
                for t, value in enumerate(values):
                    lane = slice(t * TILE, (t + 1) * TILE)
                    value = value * down_vec[2 * e : 2 * e + 1, lane] + down_vec[2 * e + 1 : 2 * e + 2, lane]
                    nrm[e, pl.ds(pl.multiple_of((at + i) * step, step), step), lane] = value.astype(BF16)

    def products(cells, ups, skip=0):
        size = len(cells) * step
        whole = len(ups) * size

        def down(e):
            wide = jnp.dot(nrm[e, 0:size, :], dw[e], preferred_element_type=F32)
            coarse[e * size : (e + 1) * size, :] = wide.astype(BF16)
            for i, (_, merged_col, (_, _, merged_at)) in enumerate(cells):
                if merged_col is None or merged_at is None:
                    continue
                for p in range(PAIRS):
                    at = i * step + p * sub
                    for t in range(3):
                        turn_merged[
                            merged_at + skip, (2 * p + e) * 3 + t, pl.ds(merged_col, sub, stride=half_cols), :
                        ] = wide[at : at + sub, t * TILE : (t + 1) * TILE]

        def widen(block, off, which):
            rows = slice(which[0] * size, (which[-1] + 1) * size)
            spread = jnp.dot(coarse[rows, :], uw[block], preferred_element_type=F32)
            for e in which:
                for at in range(0, size, step):
                    lo = (e - which[0]) * size + at
                    _, done = pair_norm([thirds(spread[lo : lo + step])], chan)
                    for t, value in enumerate(done[0]):
                        lane = slice(t * TILE, (t + 1) * TILE)
                        value = value * up_vec[0:1, lane] + up_vec[1:2, lane]
                        to = e * whole + off + at
                        renorm[to : to + step, lane] = value.astype(BF16)

        for which in PARITIES:
            for e in which:
                down(e)
            for u, (block, _) in enumerate(ups):
                widen(block, u * size, which)
        for a in range(2):
            two = [
                jnp.dot(
                    renorm[e * whole : (e + 1) * whole, a * TILE : (a + 2) * TILE],
                    ow_pad[e, a],
                    preferred_element_type=F32,
                )
                for e in range(2)
            ]
            for u, (_, x) in enumerate(ups):
                for i, (_, _, (_, fine_at, _)) in enumerate(cells):
                    for p in range(PAIRS):
                        at = u * size + i * step + p * sub
                        span = slice(at, at + sub)
                        trio = (
                            two[0][span, 0:TILE],
                            two[0][span, TILE : 2 * TILE] + two[1][span, 0:TILE],
                            two[1][span, TILE : 2 * TILE],
                        )
                        for t, value in enumerate(trio):
                            turn_fine[fine_at + a, 3 * p + t, pl.ds(x, sub, stride=cols), :] = value

    own_ups = [(0, 1), (1, 2)]

    def compute_own(rows):
        cells = [(2, 1, row) for row in rows]
        first_norm(cells)
        products(cells, own_ups)

    own = pl.ds(1, cols)

    with jax.named_scope("n_own"):
        first_norm([(2, 1, row) for row in inner_rows])

    with jax.named_scope("c_own"):
        products([(2, 1, row) for row in inner_rows], own_ups)

    with jax.named_scope("w_halo"):

        @pl.when(has_above)
        def _():
            down.wait_recv()

        @pl.when(has_below)
        def _():
            up.wait_recv()
            comb[own, HALO + slots : total] = bot_in[...]

        @pl.when(jnp.logical_not(has_below))
        def _():
            comb[:, HALO + slots : total] = jnp.zeros((cols + 2, HALO, sub, lanes), BF16)

        @pl.when(has_above)
        def _():
            comb[own, 0:HALO] = top_in[...]

        @pl.when(jnp.logical_not(has_above))
        def _():
            comb[:, 0:HALO] = jnp.zeros((cols + 2, HALO, sub, lanes), BF16)

    def start_wrap():
        for copy in to_west:
            copy.start()

    with jax.named_scope("w_wrap"):

        @pl.when(first)
        def _():
            pl.semaphore_wait(ready_sem.at[2], 1)

        @pl.when(first & (lat < n_lat // 2))
        def _():
            start_wrap()

    for side, x, device in ((WEST, cols - 1, east), (EAST, 0, west)):

        @pl.when(cross_lo & sends_cross(side))
        def _():
            cross(side, x, device, top_in, top_side, 10).start()

        @pl.when(cross_hi & sends_cross(side))
        def _():
            cross(side, x, device, bot_in, bot_side, 8).start()

    outer = top_rows + bottom_rows
    with jax.named_scope("c_own_outer"):
        compute_own(outer)

    odd = lax.rem(lon, 2) == 1
    side_one = jnp.where(first | (odd & jnp.logical_not(last)), EAST, WEST)
    side_two = 1 - side_one

    def spared(side):
        return takes_cross(side) & cross_lo, takes_cross(side) & cross_hi

    def arrive(side):
        x = side * (cols + 1)
        for i in range(2):
            lo, hi = spans[i]
            column(side, cols, i, east).wait_recv()
            comb[x, HALO + lo : HALO + hi] = land[side, lo:hi]
        for i in range(HALO):
            tail_side[side, i] = comb[x, count + i]

        lo_spared, hi_spared = spared(side)

        @pl.when(has_above & jnp.logical_not(lo_spared))
        def _():
            up_side(side).start()

        @pl.when(has_below & jnp.logical_not(hi_spared))
        def _():
            down_side(side).start()

    def arrive_rest(side):
        x = side * (cols + 1)
        lo, hi = spans[2]
        column(side, cols, 2, east).wait_recv()
        comb[x, HALO + lo : HALO + hi] = land[side, lo:hi]

    def corner(side):
        x = side * (cols + 1)

        @pl.when(has_above)
        def _():
            down_side(side).wait_recv()
            comb[x, 0:HALO] = top_side[side]

        @pl.when(has_below)
        def _():
            up_side(side).wait_recv()
            comb[x, HALO + slots : total] = bot_side[side]

    def ready(row):
        _, fine_at, _ = row
        return fine_at - 2 * TOP >= mid_hi

    early = [row for row in inner_rows if ready(row)]
    late = [row for row in inner_rows if not ready(row)]
    side_rows = early + late + outer
    assert len(late) == len(outer)

    def place_of(rows):
        return [row[1] for row in side_rows].index(rows[0][1])

    def norm_side(side, rows):
        first_norm([(side * cols, 0, row) for row in rows], place_of(rows))

    def finish_side(side):
        cells = [(side * cols, 0, row) for row in side_rows]
        products(cells, [(1 - side, side * (cols - 1))], side * (blank + 1))

    hasty = first & (lax.rem(lat, 2) == 1)
    with jax.named_scope("w_one"):
        arrive(side_one)
        arrive_rest(side_one)
    with jax.named_scope("n_one"):
        norm_side(side_one, early)
        norm_side(side_one, late)
    @pl.when(first & (lat >= n_lat // 2))
    def _():
        start_wrap()

    with jax.named_scope("w_hasty"):

        @pl.when(hasty)
        def _():
            arrive(side_two)

    with jax.named_scope("k_one"):
        corner(side_one)
    with jax.named_scope("c_one"):
        norm_side(side_one, outer)
        finish_side(side_one)
    with jax.named_scope("w_two"):

        @pl.when(jnp.logical_not(hasty))
        def _():
            arrive(side_two)

    with jax.named_scope("n_two"):
        norm_side(side_two, early)

    def chosen(own, other):
        spots = [[jnp.where(hasty, x, y) for x, y in zip(a[0], b[0])] for a, b in zip(own, other)]
        at = jnp.where(hasty, place_of(own), place_of(other))
        first_norm([(side_two * cols, 0, (spot, None, None)) for spot in spots], at)

    @pl.when(hasty)
    def _():
        arrive_rest(side_two)

    @pl.when(jnp.logical_not(hasty))
    def _():
        with jax.named_scope("k_two"):
            corner(side_two)

    with jax.named_scope("m_two"):
        chosen(late, outer)

    @pl.when(hasty)
    def _():
        with jax.named_scope("kh_two"):
            corner(side_two)

    @pl.when(jnp.logical_not(hasty))
    def _():
        with jax.named_scope("r_two"):
            arrive_rest(side_two)

    with jax.named_scope("c_two"):
        chosen(outer, late)
        finish_side(side_two)

    whole_column = comb.at[1, pl.ds(HALO, slots)]
    for side, device in ((WEST, east), (EAST, west)):
        remote(whole_column, land.at[side], side, device, 3 * side).wait_send()

    @pl.when(has_above)
    def _():
        up.wait_send()

    @pl.when(has_below)
    def _():
        down.wait_send()

    for side, x, device in ((WEST, cols - 1, east), (EAST, 0, west)):
        lo_spared, hi_spared = spared(side)

        @pl.when(has_above & jnp.logical_not(lo_spared))
        def _():
            up_side(side).wait_send()

        @pl.when(has_below & jnp.logical_not(hi_spared))
        def _():
            down_side(side).wait_send()

        @pl.when((cross_lo | cross_hi) & sends_cross(side))
        def _():
            cross(side, x, device, top_in, top_side, 10).wait_send()


def write_out(turn_merged, turn_fine, places, merged_hbm, fine_hbm, merged_buf, fine_buf, sem):
    members, merged_slots, half_cols, _ = merged_buf.shape
    _, slots, cols, packed = fine_buf.shape
    sub = turn_fine.shape[2] // cols
    halves = sub // members
    lanes = packed // halves
    inner = slots // 2 - TOP
    blank = inner + BOTTOM + TOP
    count, shift, edge, count_out = places[0], places[1], places[2], places[3]
    copies = []

    def put(turn, index, slot, buf, width, span):
        value = turn[index].astype(BF16)
        for half in range(halves):
            for member in range(members):
                at = (half * members + member) * width
                buf[member, slot, :, half * span : (half + 1) * span] = jnp.concatenate(
                    [value[t, at : at + width] for t in range(span // TILE)], axis=1
                )

    def send(buf, hbm, lo, hi):
        span = pl.ds(lo, hi - lo)
        copy = pltpu.make_async_copy(buf.at[:, span], hbm.at[:, span], sem.at[len(copies)])
        copy.start()
        copies.append(copy)

    for lo in range(0, slots, 5):
        hi = min(lo + 5, slots)
        for slot in range(lo, hi):
            r = slot + 2 * TOP - shift
            after = jnp.minimum(2 * (TOP + inner) + r - 2 * edge, 2 * (TOP + inner + BOTTOM) - 1)
            before = jnp.where(r < 2 * (TOP + inner), r, r - 2 * (TOP + inner))
            index = jnp.where(r < 2 * edge, before, after)
            index = jnp.where(slot < count, index, 2 * (TOP + inner + BOTTOM))
            put(turn_fine, index, slot, fine_buf, cols, lanes)
        send(fine_buf, fine_hbm, lo, hi)
    for lo in range(0, merged_slots, 4):
        hi = min(lo + 4, merged_slots)
        for slot in range(lo, hi):
            m = slot + TOP
            index = min(slot if slot < inner else slot + BOTTOM, blank - 1)
            index = jnp.where(m < edge, index, jnp.minimum(inner + m - edge, inner + BOTTOM - 1))
            index = jnp.where(slot < count_out, index, blank)
            put(turn_merged, index, slot, merged_buf, half_cols, 2 * lanes)
        send(merged_buf, merged_hbm, lo, hi)
    for copy in copies:
        copy.wait()


def body(
    tokens,
    in_bounds,
    out_bounds,
    down_gain,
    down_bias,
    down_weight,
    up_weight,
    up_gain,
    up_bias,
    out_weight,
):
    members, slots, cols, packed = tokens.shape
    chan = down_weight.shape[0] // 4
    halves = packed // (chan * LANES_OF_LEVELS)
    lanes = chan * LANES_OF_LEVELS
    sub = halves * members
    merged_slots = slots // 2 + 1
    half_cols = cols // 2
    inner = slots // 2 - TOP
    edges = TOP + BOTTOM
    total = slots + 2 * HALO
    most = (inner + edges) * PAIRS * sub
    wide = max(2 * inner, inner + edges) * PAIRS * sub
    n_lat = lax.axis_size("lat")
    n_lon = lax.axis_size("lon")
    vmem = pl.BlockSpec(memory_space=pltpu.VMEM)
    smem = pl.BlockSpec(memory_space=pltpu.SMEM)
    hbm = pl.BlockSpec(memory_space=pltpu.HBM)
    patch = pltpu.VMEM((cols, HALO, sub, lanes), BF16)
    corner = pltpu.VMEM((2, HALO, sub, lanes), BF16)
    operands = (
        in_bounds,
        out_bounds,
        tokens,
        down_weight,
        up_weight,
        out_weight,
        down_gain,
        down_bias,
        up_gain,
        up_bias,
    )
    merged_shape = (members, merged_slots, half_cols, 2 * packed)
    held = pl.pallas_call(
        functools.partial(kernel, n_lat, n_lon),
        out_shape=(
            pltpu.VMEM((2 * (inner + edges + 1), 2 * lanes // TILE, half_cols * sub, TILE), F32),
            pltpu.VMEM((2 * (TOP + inner + BOTTOM) + 1, lanes // TILE, cols * sub, TILE), F32),
            pltpu.SMEM((4,), jnp.int32),
        ),
        in_specs=[hbm] * 10,
        out_specs=(vmem, vmem, smem),
        scratch_shapes=[
            pltpu.VMEM((cols + 2, total, sub, lanes), BF16),
            pltpu.VMEM((2, slots, sub, lanes), BF16),
            patch,
            patch,
            corner,
            corner,
            patch,
            corner,
            pltpu.VMEM((2, most, 4 * chan), BF16),
            pltpu.VMEM((2 * most, 2 * chan), BF16),
            pltpu.VMEM((2 * wide, 2 * chan), BF16),
            pltpu.VMEM((slots, lanes // TILE, sub * cols, TILE), F32),
            pltpu.VMEM((2, *down_weight.shape), BF16),
            pltpu.VMEM((2, 2 * chan, 2 * chan), BF16),
            pltpu.VMEM(out_weight.shape, BF16),
            pltpu.VMEM((2, 2, 2 * TILE, 2 * TILE), BF16),
            pltpu.VMEM((4, 4 * chan), F32),
            pltpu.VMEM((2, 2 * chan), F32),
            pltpu.VMEM(tokens.shape, BF16),
            pltpu.SMEM(in_bounds.shape, jnp.int32),
            pltpu.SMEM(out_bounds.shape, jnp.int32),
            pltpu.VMEM(down_gain.shape, F32),
            pltpu.VMEM(down_bias.shape, F32),
            pltpu.VMEM(up_gain.shape, F32),
            pltpu.VMEM(up_bias.shape, F32),
            pltpu.SemaphoreType.DMA((5,)),
            pltpu.SemaphoreType.DMA((10,)),
            pltpu.SemaphoreType.DMA((12,)),
            pltpu.SemaphoreType.REGULAR((3,)),
        ],
        compiler_params=pltpu.CompilerParams(
            collective_id=0, has_side_effects=True, vmem_limit_bytes=48 * 2**20
        ),
    )(*[pltpu.with_memory_space_constraint(x, pltpu.HBM) for x in operands])
    spaces = (pltpu.VMEM, pltpu.VMEM, pltpu.SMEM)
    return pl.pallas_call(
        write_out,
        out_shape=(
            jax.ShapeDtypeStruct(merged_shape, BF16),
            jax.ShapeDtypeStruct(tokens.shape, BF16),
        ),
        in_specs=[vmem, vmem, smem],
        out_specs=(hbm, hbm),
        scratch_shapes=[
            pltpu.VMEM(merged_shape, BF16),
            pltpu.VMEM(tokens.shape, BF16),
            pltpu.SemaphoreType.DMA((pl.cdiv(merged_slots, 4) + pl.cdiv(slots, 5),)),
        ],
        compiler_params=pltpu.CompilerParams(vmem_limit_bytes=48 * 2**20),
    )(*[pltpu.with_memory_space_constraint(x, space) for x, space in zip(held, spaces)])


def solution(mesh):
    return jax.shard_map(
        body,
        mesh=mesh,
        in_specs=(P(None, "lat", "lon", None), P(), P(), P(), P(), P(), P(), P(), P(), P()),
        out_specs=(P(None, "lat", "lon", None), P(None, "lat", "lon", None)),
        check_vma=False,
    )
```

```python
import functools

import jax
import jax.numpy as jnp
from jax import lax
from jax.experimental import pallas as pl
from jax.experimental.pallas import tpu as pltpu
from jax.sharding import PartitionSpec as P

HALO = 3
LANES_OF_LEVELS = 4
PAIRS = LANES_OF_LEVELS // 2
TILE = 128
TOP = 2
BOTTOM = 2
WEST, EAST = 0, 1
MESH = pl.DeviceIdType.MESH
F32 = jnp.float32
BF16 = jnp.bfloat16
PARITIES = ((0, 1),)


def pair_norm(blocks, size):
    low = lax.broadcasted_iota(jnp.int32, blocks[0][0].shape, 1) < TILE // 2
    inv = 1.0 / size

    def totals(tiles):
        one, mid, two = [functools.reduce(jnp.add, group) for group in zip(*tiles)]
        first = jnp.sum(one + jnp.where(low, mid, 0.0), axis=1, keepdims=True) * inv
        second = jnp.sum(two + jnp.where(low, 0.0, mid), axis=1, keepdims=True) * inv
        return first, second

    first, second = totals(blocks)
    mid = jnp.where(low, first, second)
    off = [(one - first, both - mid, two - second) for one, both, two in blocks]
    first, second = totals([tuple(v * v for v in tiles) for tiles in off])
    first, second = lax.rsqrt(first + 1e-05), lax.rsqrt(second + 1e-05)
    mid = jnp.where(low, first, second)
    return low, [(one * first, both * mid, two * second) for one, both, two in off]


def thirds(value):
    return tuple(value[:, t * TILE : (t + 1) * TILE] for t in range(3))


def down_pieces(chan):
    short = chan - TILE
    even = [(0, b * chan, TILE) for b in range(4)] + [(0, b * chan + TILE, short) for b in range(4)]
    odd = [(1, b * chan + short, TILE) for b in range(4)] + [(1, b * chan, short) for b in (1, 0, 3, 2)]
    return even + odd


def kernel(
    n_lat,
    n_lon,
    in_b_hbm,
    out_b_hbm,
    t_hbm,
    dw_hbm,
    uw_hbm,
    ow_hbm,
    dg_hbm,
    db_hbm,
    ug_hbm,
    ub_hbm,
    turn_merged,
    turn_fine,
    places,
    comb,
    land,
    top_in,
    bot_in,
    top_side,
    bot_side,
    tail,
    tail_side,
    nrm,
    coarse,
    renorm,
    turn_in,
    dw,
    uw,
    ow,
    ow_pad,
    down_vec,
    up_vec,
    t_ref,
    in_b,
    out_b,
    dg_ref,
    db_ref,
    ug_ref,
    ub_ref,
    local_sem,
    send_sem,
    recv_sem,
    ready_sem,
):
    members, slots, cols, packed = t_ref.shape
    _, _, sub, lanes = comb.shape
    halves = sub // members
    chan = lanes // LANES_OF_LEVELS
    short = chan - TILE
    tiles = lanes // TILE
    total = slots + 2 * HALO
    half_cols = cols // 2
    inner = slots // 2 - TOP
    blank = inner + BOTTOM + TOP
    mid_lo, mid_hi = HALO, slots // 2
    lat = lax.axis_index("lat")
    lon = lax.axis_index("lon")
    east = {"lat": lat, "lon": lax.rem(lon + 1, n_lon)}
    west = {"lat": lat, "lon": lax.rem(lon + n_lon - 1, n_lon)}
    above = {"lat": jnp.maximum(lat - 1, 0), "lon": lon}
    below = {"lat": jnp.minimum(lat + 1, n_lat - 1), "lon": lon}
    has_above = lat > 0
    has_below = lat < n_lat - 1
    first = lon == 0
    last = lon == n_lon - 1
    before_last = lon == n_lon - 2

    spans = [(0, mid_lo), (mid_hi, slots), (mid_lo, mid_hi)]
    token_loads = []
    for i, (lo, hi) in enumerate(spans):
        span = pl.ds(lo, hi - lo)
        token_loads.append(pltpu.make_async_copy(t_hbm.at[:, span], t_ref.at[:, span], local_sem.at[i]))
        token_loads[i].start()

    barrier = pltpu.get_barrier_semaphore()

    @pl.when(first | last)
    def _():
        pl.semaphore_signal(barrier, inc=1, device_id=west, device_id_type=MESH)

    @pl.when(jnp.logical_not(last))
    def _():
        pl.semaphore_signal(barrier, inc=1, device_id=east, device_id_type=MESH)

    @pl.when(has_below)
    def _():
        pl.semaphore_signal(barrier, inc=1, device_id=below, device_id_type=MESH)

    pairs = [
        (in_b_hbm, in_b),
        (out_b_hbm, out_b),
        (ow_hbm, ow),
        (dg_hbm, dg_ref),
        (db_hbm, db_ref),
        (ug_hbm, ug_ref),
        (ub_hbm, ub_ref),
    ]
    free_sems = [send_sem.at[i] for i in (3, 9, 4, 5, 6, 7, 8)]
    loads = [pltpu.make_async_copy(src, dst, sem) for (src, dst), sem in zip(pairs, free_sems)]
    for load in loads:
        load.start()
    for block in range(2):
        cut = uw_hbm.at[:, pl.ds(block * 2 * chan, 2 * chan)]
        pltpu.make_async_copy(cut, uw.at[block], local_sem.at[3]).start()
    for pos, (e, start, size) in enumerate(down_pieces(chan)):
        at = sum(piece[2] for piece in down_pieces(chan)[:pos] if piece[0] == e)
        cut = dw_hbm.at[pl.ds(start, size)]
        pltpu.make_async_copy(cut, dw.at[e, pl.ds(at, size)], local_sem.at[4]).start()

    def turn_rows(lo, hi):
        for r in range(lo, hi):
            for member in range(members):
                row = t_ref[member, r].astype(F32)
                for half in range(halves):
                    at = (half * members + member) * cols
                    for t in range(tiles):
                        lane = half * lanes + t * TILE
                        turn_in[r, t, at : at + cols, :] = row[:, lane : lane + TILE]

    sent, kept = (0, cols - 1), range(1, cols - 1)

    def take_columns(lo, hi, columns):
        for x in columns:
            for r in range(lo, hi):
                for t in range(tiles):
                    comb[1 + x, HALO + r, :, t * TILE : (t + 1) * TILE] = turn_in[
                        r, t, pl.ds(x, sub, stride=cols), :
                    ].astype(BF16)

    heard = has_above.astype(jnp.int32) + jnp.logical_not(first).astype(jnp.int32)
    heard = heard + last.astype(jnp.int32) + before_last.astype(jnp.int32)
    @pl.when(heard > 0)
    def _():
        pl.semaphore_wait(barrier, heard)

    @pl.when(jnp.logical_not(first | last))
    def _():
        pl.semaphore_signal(ready_sem.at[0], inc=1, device_id=west, device_id_type=MESH)

    @pl.when(last)
    def _():
        pl.semaphore_signal(ready_sem.at[2], inc=1, device_id=east, device_id_type=MESH)

    @pl.when(has_above)
    def _():
        pl.semaphore_signal(ready_sem.at[1], inc=1, device_id=above, device_id_type=MESH)

    with jax.named_scope("w_tok"):
        token_loads[0].wait()
    turn_rows(*spans[0])
    take_columns(*spans[0], sent)

    def remote(src, dst, slot, device, landing=None):
        return pltpu.make_async_remote_copy(
            src_ref=src,
            dst_ref=dst,
            send_sem=send_sem.at[slot],
            recv_sem=recv_sem.at[slot if landing is None else landing],
            device_id=device,
            device_id_type=MESH,
        )

    def column(side, x, i, device):
        lo, hi = spans[i]
        span = pl.ds(lo, hi - lo)
        return remote(comb.at[x, pl.ds(HALO + lo, hi - lo)], land.at[side, span], side, device, 3 * side + i)

    to_east = [column(WEST, cols, i, east) for i in range(3)]
    to_west = [column(EAST, 1, i, west) for i in range(3)]
    up = remote(comb.at[pl.ds(1, cols), pl.ds(HALO, HALO)], bot_in, 2, above, 6)
    down = remote(tail, top_in, 3, below, 7)

    def up_side(side):
        return remote(land.at[side, pl.ds(0, HALO)], bot_side.at[side], 4 + side, above, 8 + side)

    def down_side(side):
        return remote(tail_side.at[side], top_side.at[side], 6 + side, below, 10 + side)

    cross_lo = has_above & (lax.rem(lat, 2) == 0)
    cross_hi = has_below & (lax.rem(lat, 2) == 1)

    def sends_cross(side):
        return jnp.where(side == WEST, lon != n_lon - 2, lon != 1)

    def takes_cross(side):
        return jnp.where(side == WEST, jnp.logical_not(last), jnp.logical_not(first))

    def cross(side, x, device, held, landed, slot):
        return pltpu.make_async_remote_copy(
            src_ref=held.at[x],
            dst_ref=landed.at[side],
            send_sem=send_sem.at[8 + side],
            recv_sem=recv_sem.at[slot + side],
            device_id=device,
            device_id_type=MESH,
        )

    def start_early(i):
        @pl.when(before_last)
        def _():
            to_east[i].start()

        @pl.when(jnp.logical_not(first))
        def _():
            to_west[i].start()

    start_early(0)
    take_columns(*spans[0], kept)

    @pl.when(has_above)
    def _():
        up.start()

    token_loads[1].wait()
    turn_rows(*spans[1])
    take_columns(*spans[1], sent)
    start_early(1)
    take_columns(*spans[1], kept)
    token_loads[2].wait()
    turn_rows(*spans[2])
    take_columns(*spans[2], sent)
    start_early(2)
    take_columns(*spans[2], kept)

    loads[0].wait()
    loads[1].wait()
    start_in = in_b[lat]
    count = in_b[lat + 1] - start_in
    shift = 2 * out_b[lat] - start_in
    past = count - shift + 2 * TOP
    edge = past // 2
    places[0] = count
    places[1] = shift
    places[2] = edge
    places[3] = out_b[lat + 1] - out_b[lat]
    for x in range(cols):
        for i in range(HALO):
            tail[x, i] = comb[1 + x, count + i]

    with jax.named_scope("w_ready"):

        @pl.when(jnp.logical_not(last | before_last))
        def _():
            pl.semaphore_wait(ready_sem.at[0], 1)
            for copy in to_east:
                copy.start()

    @pl.when(has_below)
    def _():
        pl.semaphore_wait(ready_sem.at[1], 1)
        down.start()

    for load in loads[2:]:
        load.wait()
    pltpu.make_async_copy(uw, uw, local_sem.at[3]).wait()
    pltpu.make_async_copy(dw, dw, local_sem.at[4]).wait()

    @pl.when(last)
    def _():
        for copy in to_east:
            copy.start()

    for e in range(2):
        for row, ref in ((0, dg_ref), (1, db_ref)):
            vec = ref[...][None]
            cuts = [vec[:, at : at + size] for which, at, size in down_pieces(chan) if which == e]
            down_vec[2 * e + row : 2 * e + row + 1, :] = jnp.concatenate(cuts, axis=1)
    for row, ref in ((0, ug_ref), (1, ub_ref)):
        vec = ref[...][None]
        up_vec[row : row + 1, :] = jnp.concatenate([vec, vec], axis=1)
    ow_pad[...] = jnp.zeros(ow_pad.shape, BF16)
    plain = ow[...]
    moved = jnp.concatenate([jnp.zeros((chan, short), BF16), plain], axis=1)
    for a in range(2):
        ow_pad[0, a, a * short : a * short + chan, 0:chan] = plain
        ow_pad[1, a, a * short : a * short + chan, :] = moved

    turn_fine[2 * (TOP + inner + BOTTOM)] = jnp.zeros(turn_fine.shape[1:], F32)
    turn_merged[blank] = jnp.zeros(turn_merged.shape[1:], F32)

    def place(r):
        inside = jnp.maximum(r + shift - 1, 0)
        outside = jnp.minimum(HALO + slots + r - past, total - 1)
        return jnp.where(r < past, inside, outside)

    def own_place(r):
        return r + shift - 1

    top_rows = []
    for m, instead in ((0, shift < HALO), (1, shift == 0)):
        spots = [jnp.where(instead, own_place(2 * (TOP + inner + m) + a), place(2 * m + a)) for a in range(2)]
        top_rows.append((spots, 2 * m, inner + BOTTOM + m))
    inner_rows = [([own_place(2 * m + a) for a in range(2)], 2 * m, m - TOP) for m in range(TOP, TOP + inner)]
    bottom_rows = [
        ([place(2 * (edge + i) + a) for a in range(2)], 2 * (TOP + inner + i), inner + i) for i in range(BOTTOM)
    ]
    step = PAIRS * sub

    def first_norm(cells, at=0):
        for i, (col, _, (spots, _, _)) in enumerate(cells):
            blocks = []
            for c in range(2):
                for a in range(2):
                    row = comb[col + c, spots[a]].astype(F32)
                    both = [row[:, p * 2 * chan : (p + 1) * 2 * chan] for p in range(PAIRS)]
                    blocks.append(thirds(jnp.concatenate(both, axis=0)))
            low, done = pair_norm(blocks, 4 * chan)
            even, odd = [v[0] for v in done], [v[2] for v in done]
            for b in (0, 2):
                swapped = pltpu.roll(done[b + 1][1], TILE // 2, 1)
                even.append(jnp.where(low, done[b][1], swapped))
                odd.append(jnp.where(low, swapped, done[b][1]))
            for e, values in ((0, even), (1, odd)):
                for t, value in enumerate(values):
                    lane = slice(t * TILE, (t + 1) * TILE)
                    value = value * down_vec[2 * e : 2 * e + 1, lane] + down_vec[2 * e + 1 : 2 * e + 2, lane]
                    nrm[e, pl.ds(pl.multiple_of((at + i) * step, step), step), lane] = value.astype(BF16)

    def products(cells, ups, skip=0):
        size = len(cells) * step
        whole = len(ups) * size

        def down(e):
            wide = jnp.dot(nrm[e, 0:size, :], dw[e], preferred_element_type=F32)
            coarse[e * size : (e + 1) * size, :] = wide.astype(BF16)
            for i, (_, merged_col, (_, _, merged_at)) in enumerate(cells):
                if merged_col is None or merged_at is None:
                    continue
                for p in range(PAIRS):
                    at = i * step + p * sub
                    for t in range(3):
                        turn_merged[
                            merged_at + skip, (2 * p + e) * 3 + t, pl.ds(merged_col, sub, stride=half_cols), :
                        ] = wide[at : at + sub, t * TILE : (t + 1) * TILE]

        def widen(block, off, which):
            rows = slice(which[0] * size, (which[-1] + 1) * size)
            spread = jnp.dot(coarse[rows, :], uw[block], preferred_element_type=F32)
            for e in which:
                for at in range(0, size, step):
                    lo = (e - which[0]) * size + at
                    _, done = pair_norm([thirds(spread[lo : lo + step])], chan)
                    for t, value in enumerate(done[0]):
                        lane = slice(t * TILE, (t + 1) * TILE)
                        value = value * up_vec[0:1, lane] + up_vec[1:2, lane]
                        to = e * whole + off + at
                        renorm[to : to + step, lane] = value.astype(BF16)

        for which in PARITIES:
            for e in which:
                down(e)
            for u, (block, _) in enumerate(ups):
                widen(block, u * size, which)
        for a in range(2):
            two = [
                jnp.dot(
                    renorm[e * whole : (e + 1) * whole, a * TILE : (a + 2) * TILE],
                    ow_pad[e, a],
                    preferred_element_type=F32,
                )
                for e in range(2)
            ]
            for u, (_, x) in enumerate(ups):
                for i, (_, _, (_, fine_at, _)) in enumerate(cells):
                    for p in range(PAIRS):
                        at = u * size + i * step + p * sub
                        span = slice(at, at + sub)
                        trio = (
                            two[0][span, 0:TILE],
                            two[0][span, TILE : 2 * TILE] + two[1][span, 0:TILE],
                            two[1][span, TILE : 2 * TILE],
                        )
                        for t, value in enumerate(trio):
                            turn_fine[fine_at + a, 3 * p + t, pl.ds(x, sub, stride=cols), :] = value

    own_ups = [(0, 1), (1, 2)]

    def compute_own(rows):
        cells = [(2, 1, row) for row in rows]
        first_norm(cells)
        products(cells, own_ups)

    own = pl.ds(1, cols)

    with jax.named_scope("n_own"):
        first_norm([(2, 1, row) for row in inner_rows])

    with jax.named_scope("c_own"):
        products([(2, 1, row) for row in inner_rows], own_ups)

    with jax.named_scope("w_halo"):

        @pl.when(has_above)
        def _():
            down.wait_recv()

        @pl.when(has_below)
        def _():
            up.wait_recv()
            comb[own, HALO + slots : total] = bot_in[...]

        @pl.when(jnp.logical_not(has_below))
        def _():
            comb[:, HALO + slots : total] = jnp.zeros((cols + 2, HALO, sub, lanes), BF16)

        @pl.when(has_above)
        def _():
            comb[own, 0:HALO] = top_in[...]

        @pl.when(jnp.logical_not(has_above))
        def _():
            comb[:, 0:HALO] = jnp.zeros((cols + 2, HALO, sub, lanes), BF16)

    def start_wrap():
        for copy in to_west:
            copy.start()

    with jax.named_scope("w_wrap"):

        @pl.when(first)
        def _():
            pl.semaphore_wait(ready_sem.at[2], 1)

        @pl.when(first & (lat < n_lat // 2))
        def _():
            start_wrap()

    for side, x, device in ((WEST, cols - 1, east), (EAST, 0, west)):

        @pl.when(cross_lo & sends_cross(side))
        def _():
            cross(side, x, device, top_in, top_side, 10).start()

        @pl.when(cross_hi & sends_cross(side))
        def _():
            cross(side, x, device, bot_in, bot_side, 8).start()

    outer = top_rows + bottom_rows
    with jax.named_scope("c_own_outer"):
        compute_own(outer)

    odd = lax.rem(lon, 2) == 1
    side_one = jnp.where(first | (odd & jnp.logical_not(last)), EAST, WEST)
    side_two = 1 - side_one

    def spared(side):
        return takes_cross(side) & cross_lo, takes_cross(side) & cross_hi

    def arrive(side):
        x = side * (cols + 1)
        for i in range(2):
            lo, hi = spans[i]
            column(side, cols, i, east).wait_recv()
            comb[x, HALO + lo : HALO + hi] = land[side, lo:hi]
        for i in range(HALO):
            tail_side[side, i] = comb[x, count + i]

        lo_spared, hi_spared = spared(side)

        @pl.when(has_above & jnp.logical_not(lo_spared))
        def _():
            up_side(side).start()

        @pl.when(has_below & jnp.logical_not(hi_spared))
        def _():
            down_side(side).start()

    def arrive_rest(side):
        x = side * (cols + 1)
        lo, hi = spans[2]
        column(side, cols, 2, east).wait_recv()
        comb[x, HALO + lo : HALO + hi] = land[side, lo:hi]

    def corner(side):
        x = side * (cols + 1)

        @pl.when(has_above)
        def _():
            down_side(side).wait_recv()
            comb[x, 0:HALO] = top_side[side]

        @pl.when(has_below)
        def _():
            up_side(side).wait_recv()
            comb[x, HALO + slots : total] = bot_side[side]

    def ready(row):
        _, fine_at, _ = row
        return fine_at - 2 * TOP >= mid_hi

    early = [row for row in inner_rows if ready(row)]
    late = [row for row in inner_rows if not ready(row)]
    side_rows = early + late + outer
    assert len(late) == len(outer)

    def place_of(rows):
        return [row[1] for row in side_rows].index(rows[0][1])

    def norm_side(side, rows):
        first_norm([(side * cols, 0, row) for row in rows], place_of(rows))

    def finish_side(side):
        cells = [(side * cols, 0, row) for row in side_rows]
        products(cells, [(1 - side, side * (cols - 1))], side * (blank + 1))

    hasty = first & (lax.rem(lat, 2) == 1)
    with jax.named_scope("w_one"):
        arrive(side_one)
        arrive_rest(side_one)
    with jax.named_scope("n_one"):
        norm_side(side_one, early)
        norm_side(side_one, late)
    @pl.when(first & (lat >= n_lat // 2))
    def _():
        start_wrap()

    with jax.named_scope("w_hasty"):

        @pl.when(hasty)
        def _():
            arrive(side_two)

    with jax.named_scope("k_one"):
        corner(side_one)
    with jax.named_scope("c_one"):
        norm_side(side_one, outer)
        finish_side(side_one)
    with jax.named_scope("w_two"):

        @pl.when(jnp.logical_not(hasty))
        def _():
            arrive(side_two)

    with jax.named_scope("n_two"):
        norm_side(side_two, early)

    def chosen(own, other):
        spots = [[jnp.where(hasty, x, y) for x, y in zip(a[0], b[0])] for a, b in zip(own, other)]
        at = jnp.where(hasty, place_of(own), place_of(other))
        first_norm([(side_two * cols, 0, (spot, None, None)) for spot in spots], at)

    @pl.when(hasty)
    def _():
        arrive_rest(side_two)

    @pl.when(jnp.logical_not(hasty))
    def _():
        with jax.named_scope("k_two"):
            corner(side_two)

    with jax.named_scope("m_two"):
        chosen(late, outer)

    @pl.when(hasty)
    def _():
        with jax.named_scope("kh_two"):
            corner(side_two)

    @pl.when(jnp.logical_not(hasty))
    def _():
        with jax.named_scope("r_two"):
            arrive_rest(side_two)

    with jax.named_scope("c_two"):
        chosen(outer, late)
        finish_side(side_two)

    whole_column = comb.at[1, pl.ds(HALO, slots)]
    for side, device in ((WEST, east), (EAST, west)):
        remote(whole_column, land.at[side], side, device, 3 * side).wait_send()

    @pl.when(has_above)
    def _():
        up.wait_send()

    @pl.when(has_below)
    def _():
        down.wait_send()

    for side, x, device in ((WEST, cols - 1, east), (EAST, 0, west)):
        lo_spared, hi_spared = spared(side)

        @pl.when(has_above & jnp.logical_not(lo_spared))
        def _():
            up_side(side).wait_send()

        @pl.when(has_below & jnp.logical_not(hi_spared))
        def _():
            down_side(side).wait_send()

        @pl.when((cross_lo | cross_hi) & sends_cross(side))
        def _():
            cross(side, x, device, top_in, top_side, 10).wait_send()


def write_out(turn_merged, turn_fine, places, merged_hbm, fine_hbm, merged_buf, fine_buf, sem):
    members, merged_slots, half_cols, _ = merged_buf.shape
    _, slots, cols, packed = fine_buf.shape
    sub = turn_fine.shape[2] // cols
    halves = sub // members
    lanes = packed // halves
    inner = slots // 2 - TOP
    blank = inner + BOTTOM + TOP
    count, shift, edge, count_out = places[0], places[1], places[2], places[3]
    copies = []

    def put(turn, index, slot, buf, width, span):
        value = turn[index].astype(BF16)
        for half in range(halves):
            for member in range(members):
                at = (half * members + member) * width
                buf[member, slot, :, half * span : (half + 1) * span] = jnp.concatenate(
                    [value[t, at : at + width] for t in range(span // TILE)], axis=1
                )

    def send(buf, hbm, lo, hi):
        span = pl.ds(lo, hi - lo)
        copy = pltpu.make_async_copy(buf.at[:, span], hbm.at[:, span], sem.at[len(copies)])
        copy.start()
        copies.append(copy)

    for lo in range(0, slots, 5):
        hi = min(lo + 5, slots)
        for slot in range(lo, hi):
            r = slot + 2 * TOP - shift
            after = jnp.minimum(2 * (TOP + inner) + r - 2 * edge, 2 * (TOP + inner + BOTTOM) - 1)
            before = jnp.where(r < 2 * (TOP + inner), r, r - 2 * (TOP + inner))
            index = jnp.where(r < 2 * edge, before, after)
            index = jnp.where(slot < count, index, 2 * (TOP + inner + BOTTOM))
            put(turn_fine, index, slot, fine_buf, cols, lanes)
        send(fine_buf, fine_hbm, lo, hi)
    for lo in range(0, merged_slots, 4):
        hi = min(lo + 4, merged_slots)
        for slot in range(lo, hi):
            m = slot + TOP
            index = min(slot if slot < inner else slot + BOTTOM, blank - 1)
            index = jnp.where(m < edge, index, jnp.minimum(inner + m - edge, inner + BOTTOM - 1))
            index = jnp.where(slot < count_out, index, blank)
            put(turn_merged, index, slot, merged_buf, half_cols, 2 * lanes)
        send(merged_buf, merged_hbm, lo, hi)
    for copy in copies:
        copy.wait()


def body(
    tokens,
    in_bounds,
    out_bounds,
    down_gain,
    down_bias,
    down_weight,
    up_weight,
    up_gain,
    up_bias,
    out_weight,
):
    members, slots, cols, packed = tokens.shape
    chan = down_weight.shape[0] // 4
    halves = packed // (chan * LANES_OF_LEVELS)
    lanes = chan * LANES_OF_LEVELS
    sub = halves * members
    merged_slots = slots // 2 + 1
    half_cols = cols // 2
    inner = slots // 2 - TOP
    edges = TOP + BOTTOM
    total = slots + 2 * HALO
    most = (inner + edges) * PAIRS * sub
    wide = max(2 * inner, inner + edges) * PAIRS * sub
    n_lat = lax.axis_size("lat")
    n_lon = lax.axis_size("lon")
    vmem = pl.BlockSpec(memory_space=pltpu.VMEM)
    smem = pl.BlockSpec(memory_space=pltpu.SMEM)
    hbm = pl.BlockSpec(memory_space=pltpu.HBM)
    patch = pltpu.VMEM((cols, HALO, sub, lanes), BF16)
    corner = pltpu.VMEM((2, HALO, sub, lanes), BF16)
    operands = (
        in_bounds,
        out_bounds,
        tokens,
        down_weight,
        up_weight,
        out_weight,
        down_gain,
        down_bias,
        up_gain,
        up_bias,
    )
    merged_shape = (members, merged_slots, half_cols, 2 * packed)
    held = pl.pallas_call(
        functools.partial(kernel, n_lat, n_lon),
        out_shape=(
            pltpu.VMEM((2 * (inner + edges + 1), 2 * lanes // TILE, half_cols * sub, TILE), F32),
            pltpu.VMEM((2 * (TOP + inner + BOTTOM) + 1, lanes // TILE, cols * sub, TILE), F32),
            pltpu.SMEM((4,), jnp.int32),
        ),
        in_specs=[hbm] * 10,
        out_specs=(vmem, vmem, smem),
        scratch_shapes=[
            pltpu.VMEM((cols + 2, total, sub, lanes), BF16),
            pltpu.VMEM((2, slots, sub, lanes), BF16),
            patch,
            patch,
            corner,
            corner,
            patch,
            corner,
            pltpu.VMEM((2, most, 4 * chan), BF16),
            pltpu.VMEM((2 * most, 2 * chan), BF16),
            pltpu.VMEM((2 * wide, 2 * chan), BF16),
            pltpu.VMEM((slots, lanes // TILE, sub * cols, TILE), F32),
            pltpu.VMEM((2, *down_weight.shape), BF16),
            pltpu.VMEM((2, 2 * chan, 2 * chan), BF16),
            pltpu.VMEM(out_weight.shape, BF16),
            pltpu.VMEM((2, 2, 2 * TILE, 2 * TILE), BF16),
            pltpu.VMEM((4, 4 * chan), F32),
            pltpu.VMEM((2, 2 * chan), F32),
            pltpu.VMEM(tokens.shape, BF16),
            pltpu.SMEM(in_bounds.shape, jnp.int32),
            pltpu.SMEM(out_bounds.shape, jnp.int32),
            pltpu.VMEM(down_gain.shape, F32),
            pltpu.VMEM(down_bias.shape, F32),
            pltpu.VMEM(up_gain.shape, F32),
            pltpu.VMEM(up_bias.shape, F32),
            pltpu.SemaphoreType.DMA((5,)),
            pltpu.SemaphoreType.DMA((10,)),
            pltpu.SemaphoreType.DMA((12,)),
            pltpu.SemaphoreType.REGULAR((3,)),
        ],
        compiler_params=pltpu.CompilerParams(
            collective_id=0, has_side_effects=True, vmem_limit_bytes=48 * 2**20
        ),
    )(*[pltpu.with_memory_space_constraint(x, pltpu.HBM) for x in operands])
    spaces = (pltpu.VMEM, pltpu.VMEM, pltpu.SMEM)
    return pl.pallas_call(
        write_out,
        out_shape=(
            jax.ShapeDtypeStruct(merged_shape, BF16),
            jax.ShapeDtypeStruct(tokens.shape, BF16),
        ),
        in_specs=[vmem, vmem, smem],
        out_specs=(hbm, hbm),
        scratch_shapes=[
            pltpu.VMEM(merged_shape, BF16),
            pltpu.VMEM(tokens.shape, BF16),
            pltpu.SemaphoreType.DMA((pl.cdiv(merged_slots, 4) + pl.cdiv(slots, 5),)),
        ],
        compiler_params=pltpu.CompilerParams(vmem_limit_bytes=48 * 2**20),
    )(*[pltpu.with_memory_space_constraint(x, space) for x, space in zip(held, spaces)])


def solution(mesh):
    return jax.shard_map(
        body,
        mesh=mesh,
        in_specs=(P(None, "lat", "lon", None), P(), P(), P(), P(), P(), P(), P(), P(), P()),
        out_specs=(P(None, "lat", "lon", None), P(None, "lat", "lon", None)),
        check_vma=False,
    )
```
